32 devices in a mesh: blk: 8 (over z, x), dp: 4 (over y, core).
Axes of the slice: x: 2, y: 2, z: 4, core: 2. Of those that a mesh axis runs over, the one named last changes fastest.
Arguments:
- tokens: bfloat16 [1024, 5120], P('blk', 'dp'), may hold values from -6 to 6
- expert_ids: int32 [1024, 6], P('blk'), may hold values from 0 to 15, all different within a row; in each aligned block of 128 rows (0 to 127, 128 to 255, ...) at most 96 rows name the same one
- gate_vals: float32 [1024, 6], P('blk'), may hold values from 0.1 to 1
- w_gate: bfloat16 [16, 5120, 1536], P('blk', 'dp'), may hold values from -0.078125 to 0.078125
- w_up: bfloat16 [16, 5120, 1536], P('blk', 'dp'), may hold values from -0.078125 to 0.078125
- w_down: bfloat16 [16, 5120, 1536], P('blk', 'dp'), may hold values from -0.15625 to 0.15625
Outputs:
- combined: bfloat16 [1024, 5120], P('blk', 'dp')
The draws below stay inside these ranges and needn't reach their ends.
Inputs may be any that keep to these rules, and one draw needn't show every extreme that they name: `expert_ids`: each row names 6 different experts. Among the 128 rows of one index of blk (aligned blocks) no expert is named more than 96 times, a bound that some block reaches.
All inputs are finite; a program needn't handle non-finite values.
Results may differ from the reference program's by a relative error of at most 0.0057.
Values may be sent and summed in bfloat16 or wider, within the bound.
A program may use at most 128 MiB of HBM per device.

```python
import math
import jax
import jax.numpy as jnp
import numpy as np
from jax import lax

D = 5120
FF = 1536
TOP = 6
TOK_DEV = 128
EXPERTS = 16
TOKENS = 1024
CAP = 96
N_BLK = 8


def levels(rng, shape, shards, low, top_value):
    factor_of = 1.0
    for dim, parts in shards:
        steps = jax.random.uniform(jax.random.fold_in(jax.random.fold_in(rng, 6), dim), (parts,), jnp.float32, low / len(shards), top_value / len(shards))
        factor_of = factor_of * jnp.repeat(jnp.exp(steps), shape[dim] // parts).reshape((-1,) + (1,) * (len(shape) - 1 - dim))
    return factor_of


def deal_out(rng, own, number, rows, count, top, bound, slope):
    ranking = jax.random.permutation(rng, count)
    packed, ordinary = load_shares(count, rows * top, bound, slope, True), load_shares(count, rows * top, bound, slope, False)
    places = jnp.arange(count)

    def named(tallies, turn):
        used = int((tallies > 0).sum())
        fixed = max(1, used // 4)
        moved = fixed + (places - fixed + turn * (used - fixed)) % max(1, count - fixed)
        return jnp.zeros((count,), jnp.int32).at[ranking[jnp.where(places < fixed, places, moved)]].set(jnp.asarray(tallies, jnp.int32))

    tallies = jnp.where(number % 4 == 0, named(packed, number // 4), named(ordinary, number - number // 4 - 1))
    mixed = jax.random.permutation(jax.random.fold_in(own, 3), count)
    source_of, taker = mixed[0:count // 2 * 2:2], mixed[1:count // 2 * 2:2]
    room = jnp.minimum(tallies[source_of] - 1, bound - tallies[taker]) // 2
    room = jnp.where((source_of == ranking[0]) | (taker == ranking[0]) | (tallies[taker] == 0), 0, jnp.maximum(room, 0))
    moved = jax.random.randint(jax.random.fold_in(own, 4), (count // 2,), 0, 1 << 20) % (room + 1)
    tallies = tallies.at[source_of].add(-moved).at[taker].add(moved)
    items = jnp.searchsorted(jnp.cumsum(tallies), jnp.arange(rows * top), side="right").astype(jnp.int32)
    grid = items.reshape(top, rows).T
    grid = grid[jax.random.permutation(jax.random.fold_in(own, 1), rows)]
    turn = jax.random.randint(jax.random.fold_in(own, 2), (rows, 1), 0, top)
    return jnp.take_along_axis(grid, (jnp.arange(top)[None, :] + turn) % top, axis=1)


def load_shares(amount, total, most, slope, full):
    loads = [(1 << 20) // math.isqrt(rank ** slope) + 1 for rank in range(1, amount + 1)]
    largest = most if full else min(most, max(-(-total // amount), total * loads[0] // sum(loads)))
    least = 1 if total - largest >= amount - 1 else 0
    counts, spare = [largest] + [least] * (amount - 1), total - largest - least * (amount - 1)
    while spare > 0:
        free = [i for i in range(1, amount) if counts[i] < largest] or [i for i in range(1, amount) if counts[i] < most]
        pool, remaining = sum([loads[i] for i in free]), spare
        for i in free:
            more = min(most - counts[i], max(1, remaining * loads[i] // pool), spare)
            counts[i] = counts[i] + more
            spare = spare - more
    return np.array(counts)


def gaussian(key, extent, deviation, most, split=(), held_as=jnp.bfloat16):
    array = jax.random.normal(key, extent, jnp.float32) * deviation
    if len(split) > 0:
        array = levels(key, extent, split, -0.22, 0.18) * array
    return jnp.clip(array, min=-most, max=most).astype(held_as)


def setup_inputs(seed: int = 0) -> dict:
    streams_of = jax.random.split(jax.random.key(seed), 7)
    tokens = gaussian(streams_of[0], (TOKENS, D), 1.0, 6.0, ((0, 8), (1, 4)))
    expert_ids_keys = jax.random.split(jax.random.fold_in(streams_of[1], 1), TOKENS // TOK_DEV)
    expert_ids_turns = jax.random.permutation(jax.random.fold_in(streams_of[1], 3), TOKENS // TOK_DEV)
    expert_ids = jax.vmap(lambda own, number: deal_out(jax.random.fold_in(streams_of[1], 2), own, number, TOK_DEV, EXPERTS, TOP, CAP, 2))(expert_ids_keys, expert_ids_turns).reshape((TOKENS, TOP))
    gate_vals = jnp.clip(jnp.exp(math.log(1.0) - 2.3025851 * jax.random.uniform(streams_of[2], (TOKENS, TOP), jnp.float32) ** levels(streams_of[2], (TOKENS, TOP), ((0, 8),), -0.2, 0.2)), 0.1, 1.0)
    w_gate = gaussian(streams_of[3], (EXPERTS, D, FF), D ** -0.5, 0.078125, ((0, 8), (1, 4)))
    w_up = gaussian(streams_of[4], (EXPERTS, D, FF), D ** -0.5, 0.078125, ((0, 8), (1, 4)))
    w_down = gaussian(streams_of[5], (EXPERTS, D, FF), FF ** -0.5, 0.15625, ((0, 8), (1, 4)))
    return dict(tokens=tokens, expert_ids=expert_ids, gate_vals=gate_vals, w_gate=w_gate, w_up=w_up, w_down=w_down)


def reference(tokens, expert_ids, gate_vals, w_gate, w_up, w_down):
    rows_all = N_BLK * CAP
    pairs = expert_ids.reshape(N_BLK, TOK_DEV * TOP)
    onehot = (pairs[:, :, None] == jnp.arange(EXPERTS, dtype=jnp.int32)[None, None, :]).astype(jnp.int32)
    before = jnp.cumsum(onehot, axis=1) - onehot
    position = jnp.sum(before * onehot, axis=2).astype(jnp.int32)
    source = jnp.arange(N_BLK, dtype=jnp.int32)[:, None]
    slot_index = (pairs * rows_all + source * CAP + position).reshape(-1).astype(jnp.int32)
    copies = jnp.repeat(tokens, TOP, axis=0)
    buffer = jnp.zeros((EXPERTS * rows_all, D), tokens.dtype).at[slot_index].set(copies)
    buffer = buffer.reshape(EXPERTS, rows_all, D)

    def expert_fn(items):
        row_block, gate_w, up_w, down_w = items
        gate_part = jnp.dot(row_block, gate_w, preferred_element_type=jnp.float32)
        up_part = jnp.dot(row_block, up_w, preferred_element_type=jnp.float32)
        hidden = (jax.nn.silu(gate_part) * up_part).astype(jnp.bfloat16)
        output = lax.dot_general(hidden, down_w, (((1,), (1,)), ((), ())), preferred_element_type=jnp.float32)
        return output.astype(jnp.bfloat16)

    outputs = lax.map(expert_fn, (buffer, w_gate, w_up, w_down)).reshape(EXPERTS * rows_all, D)
    picked = outputs[slot_index].astype(jnp.float32).reshape(TOKENS, TOP, D)
    combined = jnp.sum(picked * gate_vals[:, :, None], axis=1)
    return combined.astype(jnp.bfloat16)
```

```python
import functools

import jax
import jax.numpy as jnp
from jax import lax
from jax.experimental import pallas as pl
from jax.experimental.pallas import tpu as pltpu
from jax.sharding import PartitionSpec as P

MESH = pl.DeviceIdType.MESH
VMEM_BYTES = 66_000_000
TILE = 384
DOWN = 256


def flip(a, m, size):
    total, unit = 0, 1
    while unit < size:
        total = total + lax.rem(lax.div(a, unit) + lax.div(m, unit), 2) * unit
        unit *= 2
    return total


def fused_kernel(
    n_blk, tok_ref, info_ref, wg_hbm, wu_hbm, wd_hbm, out_ref,
    wg, wu, wd, everyone, routed, part, near, far_out, far_in, hidden, rows_out,
    outgoing, arrived, hold, acc, info, high, low, hot,
    w_sem, tok_s, tok_r, near_s, near_r, far_s, far_r, hy_s, hy_r, hc_s, hc_r, hf_s, hf_r, ret_s, ret_r, info_s, info_r,
):
    blk = lax.axis_index("blk")
    dp = lax.axis_index("dp")
    y, c = lax.div(dp, 2), lax.rem(dp, 2)
    mate = (blk, y * 2 + (1 - c))
    across = (blk, (1 - y) * 2 + c)
    held, width, ff = wg.shape
    cols = ff // 2
    half = near.shape[2]
    cap = 2 * half
    units = held * n_blk

    def copy(src, dst, send, recv, device):
        return pltpu.make_async_remote_copy(
            src_ref=src, dst_ref=dst, send_sem=send, recv_sem=recv,
            device_id=device, device_id_type=MESH,
        )

    def peer(m):
        return (flip(blk, m, n_blk), dp)

    def mask_of(i):
        m = jnp.where(i == 0, 0, jnp.where(i == 1, 2, i + 2))
        return jnp.where(i == n_blk - 2, 3, jnp.where(i == n_blk - 1, 1, m))

    def tok_direct(m):
        return copy(tok_ref, everyone.at[m], tok_s.at[m], tok_r.at[m], peer(m))

    def info_direct(m):
        return copy(info_ref, info.at[m], info_s.at[m], info_r.at[m], peer(m))

    def tok_onward(m):
        return copy(everyone.at[m], everyone.at[m + 1], tok_s.at[m + 1], tok_r.at[m + 1], peer(1))

    def near_copy(u):
        return copy(part.at[0], near.at[u], near_s.at[u], near_r.at[u], mate)

    def far_copy(u):
        return copy(far_out.at[u], far_in.at[u], far_s.at[u], far_r.at[u], across)

    def hidden_far(u):
        return copy(hidden.at[u, c, y], hidden.at[u, c, y], hy_s.at[u], hy_r.at[u], across)

    def hidden_near(u):
        return copy(hidden.at[u, c, y], hidden.at[u, c, y], hc_s.at[u], hc_r.at[u], mate)

    def hidden_onward(u):
        return copy(hidden.at[u, c, 1 - y], hidden.at[u, c, 1 - y], hf_s.at[u], hf_r.at[u], mate)

    def ret_copy(m):
        to = jnp.where(lax.rem(m, 2) == 1, 1, m)
        return copy(outgoing.at[m], arrived.at[m], ret_s.at[m], ret_r.at[m], peer(to))

    def load(k, h):
        hbm, vmem = ((wg_hbm, wg), (wu_hbm, wu), (wd_hbm, wd))[k]
        return pltpu.make_async_copy(hbm.at[h], vmem.at[h], w_sem.at[k, h])

    load(0, 0).start()
    load(1, 0).start()

    barrier = pltpu.get_barrier_semaphore()
    for m in range(1, n_blk):
        pl.semaphore_signal(barrier, inc=1, device_id=peer(m), device_id_type=MESH)
    for device in (mate, across):
        pl.semaphore_signal(barrier, inc=1, device_id=device, device_id_type=MESH)
    pl.semaphore_wait(barrier, n_blk + 1)

    for m in range(1, n_blk):
        info_direct(m).start()
    for m in [1] + list(range(2, n_blk - 2, 2)):
        tok_direct(m).start()
    everyone[0] = tok_ref[...]
    info[0] = info_ref[...]
    tok_rows = tok_ref.shape[0]
    lines = info_ref.shape[0] // 2

    def slots_of(m):
        square = (tok_rows, tok_rows)
        before = lax.broadcasted_iota(jnp.int32, square, 0) < lax.broadcasted_iota(jnp.int32, square, 1)
        before = jnp.where(before, 1.0, 0.0).astype(jnp.bfloat16)
        slot = lax.broadcasted_iota(jnp.int32, (cap, tok_rows), 0).astype(jnp.float32)
        ids, gates = info[m, :lines], info[m, lines:]
        for h in range(held):
            match = ids == (held * blk + h).astype(jnp.float32)
            member = jnp.sum(jnp.where(match, 1.0, 0.0), axis=0, keepdims=True)
            weight = jnp.sum(jnp.where(match, gates, 0.0), axis=0, keepdims=True)
            wide = jnp.broadcast_to(member, (16, tok_rows)).astype(jnp.bfloat16)
            position = jnp.dot(wide, before, preferred_element_type=jnp.float32)[0:1]
            taken = (slot == position) & (member > 0.5)
            weighted = jnp.where(taken, weight, 0.0)
            top = weighted.astype(jnp.bfloat16)
            span = slice(h * cap, (h + 1) * cap)
            high[m, span, :] = top
            low[m, span, :] = (weighted - top.astype(jnp.float32)).astype(jnp.bfloat16)
            hot[h] = jnp.where(taken, 1.0, 0.0).astype(jnp.bfloat16)

    def project(u):
        i, h = lax.div(u, held), lax.rem(u, held)
        m = mask_of(i)

        @pl.when(h == 0)
        def _():
            @pl.when(i > 0)
            def _():
                info_direct(m).wait_recv()

                @pl.when((lax.rem(m, 2) == 1) | (m == 2))
                def _():
                    tok_direct(m).wait_recv()

                @pl.when(m == 2)
                def _():
                    tok_onward(m).start()

            slots_of(m)

        routed[...] = jnp.dot(
            hot[h], everyone[m], preferred_element_type=jnp.float32
        ).astype(jnp.bfloat16)

        @pl.when(i == 0)
        def _():
            load(0, h).wait()
            load(1, h).wait()

            @pl.when(h == 0)
            def _():
                load(0, 1).start()
                load(1, 1).start()

            @pl.when(h == 1)
            def _():
                load(2, 0).start()
                load(2, 1).start()

        for side in range(2):
            first = jnp.where(c == side, cols, 0)
            for which, w in enumerate((wg, wu)):
                for f in range(0, cols, TILE):
                    at = pl.multiple_of(first + f, 128)
                    got = jnp.dot(
                        routed[...], w[h, :, pl.ds(at, TILE)], preferred_element_type=jnp.float32
                    )
                    span = slice(which * cols + f, which * cols + f + TILE)
                    part[side, 0, :, span] = got[:half]
                    part[side, 1, :, span] = got[half:]
            if side == 0:
                near_copy(u).start()

    def join(u):
        near_copy(u).wait()
        far_out[u] = (part[1, 1 - y] + near[u, 1 - y]).astype(jnp.bfloat16)
        far_copy(u).start()
        near[u, y] = near[u, y] + part[1, y]

    def activate(u):
        far_copy(u).wait_recv()
        gate = near[u, y, :, :cols] + far_in[u, :, :cols].astype(jnp.float32)
        up = near[u, y, :, cols:] + far_in[u, :, cols:].astype(jnp.float32)
        hidden[u, c, y] = (gate / (1.0 + jnp.exp(-gate)) * up).astype(jnp.bfloat16)
        hidden_far(u).start()
        hidden_near(u).start()

    def relay(u):
        hidden_far(u).wait_recv()
        hidden_onward(u).start()

    def finish(u):
        i, h = lax.div(u, held), lax.rem(u, held)
        m = mask_of(i)

        @pl.when(i == 0)
        def _():
            load(2, h).wait()

        hidden_near(u).wait_recv()
        hidden_onward(u).wait_recv()
        rows = jnp.concatenate([hidden[u, k].reshape(cap, cols) for k in range(2)], axis=1)
        for d in range(0, width, DOWN):
            rows_out[h, :, d:d + DOWN] = lax.dot_general(
                rows, wd[h, d:d + DOWN, :], (((1,), (1,)), ((), ())),
                preferred_element_type=jnp.float32,
            ).astype(jnp.bfloat16)

        @pl.when(h == held - 1)
        def _():
            both = rows_out[...].reshape(held * cap, width)
            over_slots = (((0,), (0,)), ((), ()))
            mixed = lax.dot_general(high[m], both, over_slots, preferred_element_type=jnp.float32)
            mixed = mixed + lax.dot_general(
                low[m], both, over_slots, preferred_element_type=jnp.float32
            )

            @pl.when(m == 0)
            def _():
                acc[...] = mixed

            @pl.when((m > 0) & (lax.rem(m, 2) == 0))
            def _():
                hold[lax.div(m, 2) - 1] = mixed

            @pl.when(lax.rem(m, 2) == 1)
            def _():
                outgoing[m] = mixed.astype(jnp.bfloat16)
                ret_copy(m).start()

    def spread(u):
        @pl.when(u == 3)
        def _():
            tok_direct(n_blk - 2).start()

        m = mask_of(jnp.minimum(lax.div(u + 1, held), n_blk - 1))

        @pl.when((lax.rem(u, held) == held - 1) & (m > 2) & (lax.rem(m, 2) == 0))
        def _():
            tok_direct(m).wait_recv()
            tok_onward(m).start()

    def merge(u):
        i = lax.div(u, held)
        m = mask_of(jnp.maximum(i - 1, 0)) - 1

        @pl.when((lax.rem(u, held) == held - 1) & (m > 0) & (lax.rem(m, 2) == 0))
        def _():
            ret_copy(m + 1).wait_recv()
            outgoing[m] = (hold[lax.div(m, 2) - 1] + arrived[m + 1].astype(jnp.float32)).astype(jnp.bfloat16)
            ret_copy(m).start()

    stages = ((1, join), (0, project), (2, activate), (3, relay), (4, finish), (0, spread), (4, merge))

    def step(s, carry):
        for lag, stage in stages:
            @pl.when((s >= lag) & (s - lag < units))
            def _():
                stage(s - lag)
        return carry

    lax.fori_loop(0, units + 4, step, 0)

    for m in [4, 6, 1, 2]:
        ret_copy(m).wait_recv()
        acc[...] += arrived[m].astype(jnp.float32)
    out_ref[...] = acc[...].astype(jnp.bfloat16)

    def drain(u, carry):
        far_copy(u).wait_send()
        hidden_far(u).wait_send()
        hidden_near(u).wait_send()
        hidden_onward(u).wait_send()
        return carry

    def drain_blocks(m, carry):
        info_direct(m).wait_send()
        tok_direct(m).wait_send()
        ret_copy(m).wait_send()
        return carry

    lax.fori_loop(0, units, drain, 0)
    lax.fori_loop(1, n_blk, drain_blocks, 0)


def fused(tokens, expert_ids, gate_vals, w_gate, w_up, w_down):
    n_blk = lax.axis_size("blk")
    tok_rows, width = tokens.shape
    held, _, ff = w_gate.shape
    capacity = 2 * tok_rows * expert_ids.shape[1] // (held * n_blk)
    half, units = capacity // 2, held * n_blk
    top_k = expert_ids.shape[1]
    spare = ((0, -top_k % 8), (0, 0))
    ids = jnp.pad(expert_ids.T.astype(jnp.float32), spare, constant_values=-1.0)
    packed = jnp.concatenate((ids, jnp.pad(gate_vals.T, spare)), axis=0)
    bf, f32 = jnp.bfloat16, jnp.float32
    dma = pltpu.SemaphoreType.DMA
    counts = [n_blk] * 2 + [units] * 10 + [n_blk] * 4
    vmem = pl.BlockSpec(memory_space=pltpu.VMEM)
    anywhere = pl.BlockSpec(memory_space=pl.ANY)
    return pl.pallas_call(
        functools.partial(fused_kernel, n_blk),
        out_shape=jax.ShapeDtypeStruct((tok_rows, width), bf),
        in_specs=[vmem] * 2 + [anywhere] * 3,
        out_specs=vmem,
        scratch_shapes=[
            pltpu.VMEM(w_gate.shape, bf),
            pltpu.VMEM(w_up.shape, bf),
            pltpu.VMEM(w_down.shape, bf),
            pltpu.VMEM((n_blk, tok_rows, width), bf),
            pltpu.VMEM((capacity, width), bf),
            pltpu.VMEM((2, 2, half, ff), f32),
            pltpu.VMEM((units, 2, half, ff), f32),
            pltpu.VMEM((units, half, ff), bf),
            pltpu.VMEM((units, half, ff), bf),
            pltpu.VMEM((units, 2, 2, half, ff // 2), bf),
            pltpu.VMEM((held, capacity, width), bf),
            pltpu.VMEM((n_blk, tok_rows, width), bf),
            pltpu.VMEM((n_blk, tok_rows, width), bf),
            pltpu.VMEM((n_blk // 2 - 1, tok_rows, width), f32),
            pltpu.VMEM((tok_rows, width), f32),
            pltpu.VMEM((n_blk,) + packed.shape, f32),
            pltpu.VMEM((n_blk, held * capacity, tok_rows), bf),
            pltpu.VMEM((n_blk, held * capacity, tok_rows), bf),
            pltpu.VMEM((held, capacity, tok_rows), bf),
            dma((3, held)),
        ] + [dma((count,)) for count in counts],
        compiler_params=pltpu.CompilerParams(
            collective_id=0, has_side_effects=True, vmem_limit_bytes=VMEM_BYTES
        ),
    )(tokens, packed, w_gate, w_up, w_down)


def routing(expert_ids, gate_vals, held_count, capacity):
    first = lax.axis_index("blk") * held_count
    top_k = expert_ids.shape[1]
    both = jnp.concatenate((expert_ids.astype(jnp.float32), gate_vals), axis=1)
    both = lax.all_gather(both, "blk", axis=0, tiled=False)
    ids, gates = both[:, :, :top_k].astype(jnp.int32), both[:, :, top_k:]
    mine = first + jnp.arange(held_count, dtype=jnp.int32)
    match = ids[:, None, :, :] == mine[None, :, None, None]
    member = jnp.any(match, axis=3)
    weight = jnp.sum(jnp.where(match, gates[:, None], 0.0), axis=3)
    tok_rows = ids.shape[1]
    earlier = jnp.triu(jnp.ones((tok_rows, tok_rows), jnp.float32), 1)
    position = jnp.einsum(
        "bht,tu->bhu", member.astype(jnp.bfloat16), earlier.astype(jnp.bfloat16),
        preferred_element_type=jnp.float32,
    )
    slots = jnp.arange(capacity, dtype=jnp.int32).astype(jnp.float32)
    hot = member[:, :, None, :] & (position[:, :, None, :] == slots[None, None, :, None])
    return hot.astype(jnp.bfloat16), jnp.where(hot, weight[:, :, None, :], 0.0)


def local(tokens, expert_ids, gate_vals, w_gate, w_up, w_down):
    blk_size = lax.axis_size("blk")
    tok_rows, width_dev = tokens.shape
    top_k = expert_ids.shape[1]
    held_count = w_gate.shape[0]
    capacity = 2 * tok_rows * top_k // (held_count * blk_size)
    hot, weighted = routing(expert_ids, gate_vals, held_count, capacity)
    everyone = lax.all_gather(tokens, "blk", axis=0, tiled=False)
    routed = jnp.einsum("bhpt,btd->hbpd", hot, everyone, preferred_element_type=jnp.float32)
    routed = routed.astype(jnp.bfloat16).reshape(held_count, blk_size * capacity, width_dev)
    gate_part = jnp.einsum("emd,edf->emf", routed, w_gate, preferred_element_type=jnp.float32)
    up_part = jnp.einsum("emd,edf->emf", routed, w_up, preferred_element_type=jnp.float32)
    both = jnp.stack((gate_part, up_part), axis=0)
    summed = lax.psum_scatter(both, "dp", scatter_dimension=2, tiled=True)
    hidden = (jax.nn.silu(summed[0]) * summed[1]).astype(jnp.bfloat16)
    hidden = lax.all_gather(hidden, "dp", axis=1, tiled=True)
    result = jnp.einsum("emf,edf->emd", hidden, w_down, preferred_element_type=jnp.float32)
    result = result.astype(jnp.bfloat16).reshape(held_count, blk_size, capacity, width_dev)
    high = weighted.astype(jnp.bfloat16)
    low = (weighted - high.astype(jnp.float32)).astype(jnp.bfloat16)
    partial = jnp.einsum(
        "bhpt,hbpd->btd", high, result, preferred_element_type=jnp.float32
    ) + jnp.einsum("bhpt,hbpd->btd", low, result, preferred_element_type=jnp.float32)
    partial = partial.astype(jnp.bfloat16).reshape(blk_size * tok_rows, width_dev)
    return lax.psum_scatter(partial, "blk", scatter_dimension=0, tiled=True)


def choose(tokens, expert_ids, gate_vals, w_gate, w_up, w_down):
    n_blk, held = lax.axis_size("blk"), w_gate.shape[0]
    capacity = 2 * tokens.shape[0] * expert_ids.shape[1] // (held * n_blk)
    fits = lax.axis_size("dp") == 4 and held == 2 and n_blk == 8 and capacity % 32 == 0
    fits = fits and w_gate.shape[2] % (2 * TILE) == 0 and tokens.shape[1] % DOWN == 0
    body = fused if fits else local
    return body(tokens, expert_ids, gate_vals, w_gate, w_up, w_down)


def solution(mesh):
    return jax.shard_map(
        choose,
        mesh=mesh,
        in_specs=(
            P("blk", "dp"),
            P("blk", None),
            P("blk", None),
            P("blk", "dp", None),
            P("blk", "dp", None),
            P("blk", "dp", None),
        ),
        out_specs=P("blk", "dp"),
        check_vma=False,
    )
```

```python
import functools

import jax
import jax.numpy as jnp
from jax import lax
from jax.experimental import pallas as pl
from jax.experimental.pallas import tpu as pltpu
from jax.sharding import PartitionSpec as P

MESH = pl.DeviceIdType.MESH
VMEM_BYTES = 66_000_000
TILE = 384
DOWN = 256
ORDER = (0, 2, 4, 5, 7, 6, 1, 3)


def flip(a, m, size):
    total, unit = 0, 1
    while unit < size:
        total = total + lax.rem(lax.div(a, unit) + lax.div(m, unit), 2) * unit
        unit *= 2
    return total


def fused_kernel(
    n_blk, tok_ref, ids_ref, gates_ref, wg_hbm, wu_hbm, wd_hbm, out_ref,
    wg, wu, wd, everyone, routed, part, near, far_out, far_in, hidden, rows_out,
    outgoing, arrived, hold, acc, info, high, low, hot,
    w_sem, tok_s, tok_r, near_s, near_r, far_s, far_r, hy_s, hy_r, hc_s, hc_r, hf_s, hf_r, ret_s, ret_r, info_s, info_r,
):
    blk = lax.axis_index("blk")
    dp = lax.axis_index("dp")
    y, c = lax.div(dp, 2), lax.rem(dp, 2)
    mate = (blk, y * 2 + (1 - c))
    across = (blk, (1 - y) * 2 + c)
    held, width, ff = wg.shape
    cols = ff // 2
    half = near.shape[2]
    cap = 2 * half
    units = held * n_blk

    def copy(src, dst, send, recv, device):
        return pltpu.make_async_remote_copy(
            src_ref=src, dst_ref=dst, send_sem=send, recv_sem=recv,
            device_id=device, device_id_type=MESH,
        )

    def peer(m):
        return (flip(blk, m, n_blk), dp)

    def mask_of(i):
        m = 0
        for k in range(1, n_blk):
            m = jnp.where(i == k, ORDER[k], m)
        return m

    def tok_direct(m):
        return copy(tok_ref, everyone.at[m], tok_s.at[m], tok_r.at[m], peer(m))

    def info_direct(m):
        return copy(info.at[0], info.at[m], info_s.at[m], info_r.at[m], peer(m))

    def tok_relay(have, m, k, to):
        return copy(everyone.at[have], everyone.at[m], tok_s.at[k], tok_r.at[m], peer(to))

    def tok_onward(m):
        return tok_relay(m, m + 1, m + 1, 1)

    def tok_middle():
        return copy(tok_ref, everyone.at[6], tok_s.at[0], tok_r.at[6], peer(6))

    relays = ((2, 4, 4, 6), (6, 4, 6, 2), (4, 6, n_blk, 2))

    def near_copy(u):
        return copy(part.at[0], near.at[u], near_s.at[u], near_r.at[u], mate)

    def far_copy(u):
        return copy(far_out.at[u], far_in.at[u], far_s.at[u], far_r.at[u], across)

    def hidden_far(u):
        return copy(hidden.at[u, c, y], hidden.at[u, c, y], hy_s.at[u], hy_r.at[u], across)

    def hidden_near(u):
        return copy(hidden.at[u, c, y], hidden.at[u, c, y], hc_s.at[u], hc_r.at[u], mate)

    def hidden_onward(u):
        return copy(hidden.at[u, c, 1 - y], hidden.at[u, c, 1 - y], hf_s.at[u], hf_r.at[u], mate)

    def ret_copy(m):
        to = jnp.where((lax.rem(m, 2) == 1) & (m > 3), 1, m)
        return copy(outgoing.at[m], arrived.at[m], ret_s.at[m], ret_r.at[m], peer(to))

    def load(k, h):
        hbm, vmem = ((wg_hbm, wg), (wu_hbm, wu), (wd_hbm, wd))[k]
        return pltpu.make_async_copy(hbm.at[h], vmem.at[h], w_sem.at[k, h])

    load(0, 0).start()
    load(1, 0).start()

    tok_rows = tok_ref.shape[0]
    top_k = ids_ref.shape[0]
    lines = info.shape[1] // 2
    inner = lax.rem(lax.div(lax.div(blk, 2) + 1, 2), 2) == 1
    info[0] = jnp.full(info.shape[1:], -1.0, jnp.float32)
    info[0, :top_k] = ids_ref[...].astype(jnp.float32)
    info[0, lines:lines + top_k] = gates_ref[...]

    barrier = pltpu.get_barrier_semaphore()
    for m in range(1, n_blk):
        pl.semaphore_signal(barrier, inc=1, device_id=peer(m), device_id_type=MESH)
    for device in (mate, across):
        pl.semaphore_signal(barrier, inc=1, device_id=device, device_id_type=MESH)
    pl.semaphore_wait(barrier, n_blk + 1)

    for m in range(1, n_blk):
        info_direct(m).start()
    for m in (1, 2):
        tok_direct(m).start()

    @pl.when(inner)
    def _():
        tok_middle().start()

    everyone[0] = tok_ref[...]

    def slots_of(m):
        square = (tok_rows, tok_rows)
        before = lax.broadcasted_iota(jnp.int32, square, 0) < lax.broadcasted_iota(jnp.int32, square, 1)
        before = jnp.where(before, 1.0, 0.0).astype(jnp.bfloat16)
        slot = lax.broadcasted_iota(jnp.int32, (cap, tok_rows), 0).astype(jnp.float32)
        ids, gates = info[m, :lines], info[m, lines:]
        for h in range(held):
            match = ids == (held * blk + h).astype(jnp.float32)
            member = jnp.sum(jnp.where(match, 1.0, 0.0), axis=0, keepdims=True)
            weight = jnp.sum(jnp.where(match, gates, 0.0), axis=0, keepdims=True)
            wide = jnp.broadcast_to(member, (16, tok_rows)).astype(jnp.bfloat16)
            position = jnp.dot(wide, before, preferred_element_type=jnp.float32)[0:1]
            taken = (slot == position) & (member > 0.5)
            weighted = jnp.where(taken, weight, 0.0)
            top = weighted.astype(jnp.bfloat16)
            span = slice(h * cap, (h + 1) * cap)
            high[m, span, :] = top
            low[m, span, :] = (weighted - top.astype(jnp.float32)).astype(jnp.bfloat16)
            hot[h] = jnp.where(taken, 1.0, 0.0).astype(jnp.bfloat16)

    def project(u):
        i, h = lax.div(u, held), lax.rem(u, held)
        m = mask_of(i)

        @pl.when(h == 0)
        def _():
            @pl.when(i > 0)
            def _():
                info_direct(m).wait_recv()

                @pl.when(m != 6)
                def _():
                    tok_direct(m).wait_recv()

                @pl.when(m == 2)
                def _():
                    @pl.when(inner)
                    def _():
                        tok_relay(*relays[0]).start()
                        tok_direct(6).wait_recv()
                        tok_relay(*relays[1]).start()

                    tok_onward(2).start()

                @pl.when(m == 4)
                def _():
                    @pl.when(inner)
                    def _():
                        tok_relay(*relays[2]).start()

                    tok_onward(4).start()

                @pl.when(m == 5)
                def _():
                    @pl.when(jnp.logical_not(inner))
                    def _():
                        tok_direct(6).wait_recv()

                    tok_onward(6).start()

            slots_of(m)

        routed[...] = jnp.dot(
            hot[h], everyone[m], preferred_element_type=jnp.float32
        ).astype(jnp.bfloat16)

        @pl.when(i == 0)
        def _():
            load(0, h).wait()
            load(1, h).wait()

            @pl.when(h == 0)
            def _():
                load(0, 1).start()
                load(1, 1).start()

            @pl.when(h == 1)
            def _():
                load(2, 0).start()
                load(2, 1).start()

        for side in range(2):
            first = jnp.where(c == side, cols, 0)
            for which, w in enumerate((wg, wu)):
                for f in range(0, cols, TILE):
                    at = pl.multiple_of(first + f, 128)
                    got = jnp.dot(
                        routed[...], w[h, :, pl.ds(at, TILE)], preferred_element_type=jnp.float32
                    )
                    span = slice(which * cols + f, which * cols + f + TILE)
                    part[side, 0, :, span] = got[:half]
                    part[side, 1, :, span] = got[half:]
            if side == 0:
                near_copy(u).start()

    def join(u):
        near_copy(u).wait()
        far_out[u] = (part[1, 1 - y] + near[u, 1 - y]).astype(jnp.bfloat16)
        far_copy(u).start()
        near[u, y] = near[u, y] + part[1, y]

    def activate(u):
        far_copy(u).wait_recv()
        gate = near[u, y, :, :cols] + far_in[u, :, :cols].astype(jnp.float32)
        up = near[u, y, :, cols:] + far_in[u, :, cols:].astype(jnp.float32)
        hidden[u, c, y] = (gate / (1.0 + jnp.exp(-gate)) * up).astype(jnp.bfloat16)
        hidden_far(u).start()
        hidden_near(u).start()

    def relay(u):
        hidden_far(u).wait_recv()
        hidden_onward(u).start()

    def finish(u):
        i, h = lax.div(u, held), lax.rem(u, held)
        m = mask_of(i)

        @pl.when(i == 0)
        def _():
            load(2, h).wait()

        hidden_near(u).wait_recv()
        hidden_onward(u).wait_recv()
        rows = jnp.concatenate([hidden[u, k].reshape(cap, cols) for k in range(2)], axis=1)
        for d in range(0, width, DOWN):
            rows_out[h, :, d:d + DOWN] = lax.dot_general(
                rows, wd[h, d:d + DOWN, :], (((1,), (1,)), ((), ())),
                preferred_element_type=jnp.float32,
            ).astype(jnp.bfloat16)

        @pl.when(h == held - 1)
        def _():
            both = rows_out[...].reshape(held * cap, width)
            over_slots = (((0,), (0,)), ((), ()))
            mixed = lax.dot_general(high[m], both, over_slots, preferred_element_type=jnp.float32)
            mixed = mixed + lax.dot_general(
                low[m], both, over_slots, preferred_element_type=jnp.float32
            )

            @pl.when(m == 0)
            def _():
                acc[...] = mixed

            @pl.when((m > 2) & (lax.rem(m, 2) == 0))
            def _():
                hold[lax.div(m, 2) - 2] = mixed

            @pl.when((lax.rem(m, 2) == 1) | (m == 2))
            def _():
                outgoing[m] = mixed.astype(jnp.bfloat16)
                ret_copy(m).start()

    def merge(u):
        m = jnp.where(u == 9, 4, 6)

        @pl.when((u == 9) | (u == 11))
        def _():
            ret_copy(m + 1).wait_recv()
            total = hold[lax.div(m, 2) - 2] + arrived[m + 1].astype(jnp.float32)
            outgoing[m] = total.astype(jnp.bfloat16)
            ret_copy(m).start()

    def early(u):
        @pl.when(u == units - 3)
        def _():
            finish(u)

    def late(u):
        @pl.when(u != units - 3)
        def _():
            finish(u)

    stages = (
        (1, join), (4, early), (2, activate), (0, project), (3, relay), (4, late), (4, merge),
    )

    def step(s, carry):
        for lag, stage in stages:
            @pl.when((s >= lag) & (s - lag < units))
            def _():
                stage(s - lag)
        return carry

    lax.fori_loop(0, units + 4, step, 0)

    def gathered(total, masks):
        for m in masks:
            ret_copy(m).wait_recv()
        for m in masks:
            total = total + arrived[m].astype(jnp.float32)
        return total

    acc[...] = gathered(acc[...], range(2, n_blk, 2))
    out_ref[...] = gathered(acc[...], (1, 3)).astype(jnp.bfloat16)

    def drain(u, carry):
        far_copy(u).wait_send()
        hidden_far(u).wait_send()
        hidden_near(u).wait_send()
        hidden_onward(u).wait_send()
        return carry

    def drain_blocks(m, carry):
        info_direct(m).wait_send()
        ret_copy(m).wait_send()
        return carry

    for m in (1, 2):
        tok_direct(m).wait_send()
    for m in (2, 4, 6):
        tok_onward(m).wait_send()

    @pl.when(inner)
    def _():
        tok_middle().wait_send()
        for hop in relays:
            tok_relay(*hop).wait_send()

    lax.fori_loop(0, units, drain, 0)
    lax.fori_loop(1, n_blk, drain_blocks, 0)


def fused(tokens, expert_ids, gate_vals, w_gate, w_up, w_down):
    n_blk = lax.axis_size("blk")
    tok_rows, width = tokens.shape
    held, _, ff = w_gate.shape
    capacity = 2 * tok_rows * expert_ids.shape[1] // (held * n_blk)
    half, units = capacity // 2, held * n_blk
    top_k = expert_ids.shape[1]
    lines = top_k + -top_k % 8
    bf, f32 = jnp.bfloat16, jnp.float32
    dma = pltpu.SemaphoreType.DMA
    counts = [n_blk + 1, n_blk] + [units] * 10 + [n_blk] * 4
    vmem = pl.BlockSpec(memory_space=pltpu.VMEM)
    anywhere = pl.BlockSpec(memory_space=pl.ANY)
    return pl.pallas_call(
        functools.partial(fused_kernel, n_blk),
        out_shape=jax.ShapeDtypeStruct((tok_rows, width), bf),
        in_specs=[vmem] * 3 + [anywhere] * 3,
        out_specs=vmem,
        scratch_shapes=[
            pltpu.VMEM(w_gate.shape, bf),
            pltpu.VMEM(w_up.shape, bf),
            pltpu.VMEM(w_down.shape, bf),
            pltpu.VMEM((n_blk, tok_rows, width), bf),
            pltpu.VMEM((capacity, width), bf),
            pltpu.VMEM((2, 2, half, ff), f32),
            pltpu.VMEM((units, 2, half, ff), f32),
            pltpu.VMEM((units, half, ff), bf),
            pltpu.VMEM((units, half, ff), bf),
            pltpu.VMEM((units, 2, 2, half, ff // 2), bf),
            pltpu.VMEM((held, capacity, width), bf),
            pltpu.VMEM((n_blk, tok_rows, width), bf),
            pltpu.VMEM((n_blk, tok_rows, width), bf),
            pltpu.VMEM((n_blk // 2 - 2, tok_rows, width), f32),
            pltpu.VMEM((tok_rows, width), f32),
            pltpu.VMEM((n_blk, 2 * lines, tok_rows), f32),
            pltpu.VMEM((n_blk, held * capacity, tok_rows), bf),
            pltpu.VMEM((n_blk, held * capacity, tok_rows), bf),
            pltpu.VMEM((held, capacity, tok_rows), bf),
            dma((3, held)),
        ] + [dma((count,)) for count in counts],
        compiler_params=pltpu.CompilerParams(
            collective_id=0, has_side_effects=True, vmem_limit_bytes=VMEM_BYTES
        ),
    )(tokens, expert_ids.T, gate_vals.T, w_gate, w_up, w_down)


def routing(expert_ids, gate_vals, held_count, capacity):
    first = lax.axis_index("blk") * held_count
    top_k = expert_ids.shape[1]
    both = jnp.concatenate((expert_ids.astype(jnp.float32), gate_vals), axis=1)
    both = lax.all_gather(both, "blk", axis=0, tiled=False)
    ids, gates = both[:, :, :top_k].astype(jnp.int32), both[:, :, top_k:]
    mine = first + jnp.arange(held_count, dtype=jnp.int32)
    match = ids[:, None, :, :] == mine[None, :, None, None]
    member = jnp.any(match, axis=3)
    weight = jnp.sum(jnp.where(match, gates[:, None], 0.0), axis=3)
    tok_rows = ids.shape[1]
    earlier = jnp.triu(jnp.ones((tok_rows, tok_rows), jnp.float32), 1)
    position = jnp.einsum(
        "bht,tu->bhu", member.astype(jnp.bfloat16), earlier.astype(jnp.bfloat16),
        preferred_element_type=jnp.float32,
    )
    slots = jnp.arange(capacity, dtype=jnp.int32).astype(jnp.float32)
    hot = member[:, :, None, :] & (position[:, :, None, :] == slots[None, None, :, None])
    return hot.astype(jnp.bfloat16), jnp.where(hot, weight[:, :, None, :], 0.0)


def local(tokens, expert_ids, gate_vals, w_gate, w_up, w_down):
    blk_size = lax.axis_size("blk")
    tok_rows, width_dev = tokens.shape
    top_k = expert_ids.shape[1]
    held_count = w_gate.shape[0]
    capacity = 2 * tok_rows * top_k // (held_count * blk_size)
    hot, weighted = routing(expert_ids, gate_vals, held_count, capacity)
    everyone = lax.all_gather(tokens, "blk", axis=0, tiled=False)
    routed = jnp.einsum("bhpt,btd->hbpd", hot, everyone, preferred_element_type=jnp.float32)
    routed = routed.astype(jnp.bfloat16).reshape(held_count, blk_size * capacity, width_dev)
    gate_part = jnp.einsum("emd,edf->emf", routed, w_gate, preferred_element_type=jnp.float32)
    up_part = jnp.einsum("emd,edf->emf", routed, w_up, preferred_element_type=jnp.float32)
    both = jnp.stack((gate_part, up_part), axis=0)
    summed = lax.psum_scatter(both, "dp", scatter_dimension=2, tiled=True)
    hidden = (jax.nn.silu(summed[0]) * summed[1]).astype(jnp.bfloat16)
    hidden = lax.all_gather(hidden, "dp", axis=1, tiled=True)
    result = jnp.einsum("emf,edf->emd", hidden, w_down, preferred_element_type=jnp.float32)
    result = result.astype(jnp.bfloat16).reshape(held_count, blk_size, capacity, width_dev)
    high = weighted.astype(jnp.bfloat16)
    low = (weighted - high.astype(jnp.float32)).astype(jnp.bfloat16)
    partial = jnp.einsum(
        "bhpt,hbpd->btd", high, result, preferred_element_type=jnp.float32
    ) + jnp.einsum("bhpt,hbpd->btd", low, result, preferred_element_type=jnp.float32)
    partial = partial.astype(jnp.bfloat16).reshape(blk_size * tok_rows, width_dev)
    return lax.psum_scatter(partial, "blk", scatter_dimension=0, tiled=True)


def choose(tokens, expert_ids, gate_vals, w_gate, w_up, w_down):
    n_blk, held = lax.axis_size("blk"), w_gate.shape[0]
    capacity = 2 * tokens.shape[0] * expert_ids.shape[1] // (held * n_blk)
    fits = lax.axis_size("dp") == 4 and held == 2 and n_blk == 8 and capacity % 32 == 0
    fits = fits and w_gate.shape[2] % (2 * TILE) == 0 and tokens.shape[1] % DOWN == 0
    body = fused if fits else local
    return body(tokens, expert_ids, gate_vals, w_gate, w_up, w_down)


def solution(mesh):
    return jax.shard_map(
        choose,
        mesh=mesh,
        in_specs=(
            P("blk", "dp"),
            P("blk", None),
            P("blk", None),
            P("blk", "dp", None),
            P("blk", "dp", None),
            P("blk", "dp", None),
        ),
        out_specs=P("blk", "dp"),
        check_vma=False,
    )
```

```python
import functools

import jax
import jax.numpy as jnp
from jax import lax
from jax.experimental import pallas as pl
from jax.experimental.pallas import tpu as pltpu
from jax.sharding import PartitionSpec as P

MESH = pl.DeviceIdType.MESH
VMEM_BYTES = 66_000_000
TILE = 384
DOWN = 256
RING = 4
ORDER = (0, 2, 4, 5, 7, 6, 1, 3)


def flip(a, m, size):
    total, unit = 0, 1
    while unit < size:
        total = total + lax.rem(lax.div(a, unit) + lax.div(m, unit), 2) * unit
        unit *= 2
    return total


def fused_kernel(
    n_blk, tok_ref, ids_ref, gates_ref, wg_hbm, wu_hbm, wd_hbm, out_ref,
    wg, wu, wd, everyone, routed, part, near, far_out, far_in, hidden, rows_out,
    outgoing, arrived, hold, acc, info, high, low, hot,
    w_sem, tok_s, tok_r, near_s, near_r, far_s, far_r, hy_s, hy_r, hc_s, hc_r, hf_s, hf_r, ret_s, ret_r, info_s, info_r,
):
    blk = lax.axis_index("blk")
    dp = lax.axis_index("dp")
    y, c = lax.div(dp, 2), lax.rem(dp, 2)
    mate = (blk, y * 2 + (1 - c))
    across = (blk, (1 - y) * 2 + c)
    held, width, ff = wg.shape
    cols = ff // 2
    half = near.shape[2]
    cap = 2 * half
    units = held * n_blk

    def copy(src, dst, send, recv, device):
        return pltpu.make_async_remote_copy(
            src_ref=src, dst_ref=dst, send_sem=send, recv_sem=recv,
            device_id=device, device_id_type=MESH,
        )

    def peer(m):
        return (flip(blk, m, n_blk), dp)

    def mask_of(i):
        m = 0
        for k in range(1, n_blk):
            m = jnp.where(i == k, ORDER[k], m)
        return m

    def tok_direct(m):
        return copy(tok_ref, everyone.at[m], tok_s.at[m], tok_r.at[m], peer(m))

    def info_direct(m):
        return copy(info.at[0], info.at[m], info_s.at[m], info_r.at[m], peer(m))

    def tok_relay(have, m, k, to):
        return copy(everyone.at[have], everyone.at[m], tok_s.at[k], tok_r.at[m], peer(to))

    def tok_onward(m):
        return tok_relay(m, m + 1, m + 1, 1)

    def tok_middle():
        return copy(tok_ref, everyone.at[6], tok_s.at[0], tok_r.at[6], peer(6))

    relays = ((2, 4, 4, 6), (6, 4, 6, 2), (4, 6, n_blk, 2))

    def near_copy(u, which):
        k, span = lax.rem(u, 2), slice(which * cols, (which + 1) * cols)
        return copy(
            part.at[0, :, :, span], near.at[u, :, :, span], near_s.at[k, which], near_r.at[k, which], mate
        )

    def far_copy(u):
        return copy(far_out.at[u], far_in.at[u], far_s.at[lax.rem(u, RING)], far_r.at[lax.rem(u, RING)], across)

    def hidden_far(u):
        return copy(hidden.at[u, c, y], hidden.at[u, c, y], hy_s.at[lax.rem(u, RING)], hy_r.at[lax.rem(u, RING)], across)

    def hidden_near(u):
        return copy(hidden.at[u, c, y], hidden.at[u, c, y], hc_s.at[lax.rem(u, RING)], hc_r.at[lax.rem(u, RING)], mate)

    def hidden_onward(u):
        return copy(hidden.at[u, c, 1 - y], hidden.at[u, c, 1 - y], hf_s.at[lax.rem(u, RING)], hf_r.at[lax.rem(u, RING)], mate)

    def ret_copy(m):
        to = jnp.where((lax.rem(m, 2) == 1) & (m > 3), 1, m)
        return copy(outgoing.at[m], arrived.at[m], ret_s.at[m], ret_r.at[m], peer(to))

    def load(k, h):
        hbm, vmem = ((wg_hbm, wg), (wu_hbm, wu), (wd_hbm, wd))[k]
        return pltpu.make_async_copy(hbm.at[h], vmem.at[h], w_sem.at[k, h])

    def columns(side):
        return pl.multiple_of(jnp.where(c == side, cols, 0), 128)

    def load_side(k, side):
        hbm, vmem = ((wg_hbm, wg), (wu_hbm, wu))[k]
        span = (0, slice(None), pl.ds(columns(side), cols))
        return pltpu.make_async_copy(hbm.at[span], vmem.at[span], w_sem.at[3 + k, side])

    for side in range(2):
        for k in range(2):
            load_side(k, side).start()

    tok_rows = tok_ref.shape[0]
    top_k = ids_ref.shape[0]
    lines = info.shape[1] // 2
    inner = lax.rem(lax.div(lax.div(blk, 2) + 1, 2), 2) == 1
    info[0] = jnp.full(info.shape[1:], -1.0, jnp.float32)
    info[0, :top_k] = ids_ref[...].astype(jnp.float32)
    info[0, lines:lines + top_k] = gates_ref[...]

    barrier = pltpu.get_barrier_semaphore()
    for m in range(1, n_blk):
        pl.semaphore_signal(barrier, inc=1, device_id=peer(m), device_id_type=MESH)
    for device in (mate, across):
        pl.semaphore_signal(barrier, inc=1, device_id=device, device_id_type=MESH)
    pl.semaphore_wait(barrier, n_blk + 1)

    for m in (2, 1):
        tok_direct(m).start()

    @pl.when(inner)
    def _():
        tok_middle().start()

    for m in range(1, n_blk):
        info_direct(m).start()

    everyone[0] = tok_ref[...]

    def slots_of(m):
        square = (tok_rows, tok_rows)
        before = lax.broadcasted_iota(jnp.int32, square, 0) < lax.broadcasted_iota(jnp.int32, square, 1)
        before = jnp.where(before, 1.0, 0.0).astype(jnp.bfloat16)
        slot = lax.broadcasted_iota(jnp.int32, (cap, tok_rows), 0).astype(jnp.float32)
        ids, gates = info[m, :lines], info[m, lines:]
        for h in range(held):
            match = ids == (held * blk + h).astype(jnp.float32)
            member = jnp.sum(jnp.where(match, 1.0, 0.0), axis=0, keepdims=True)
            weight = jnp.sum(jnp.where(match, gates, 0.0), axis=0, keepdims=True)
            wide = jnp.broadcast_to(member, (16, tok_rows)).astype(jnp.bfloat16)
            position = jnp.dot(wide, before, preferred_element_type=jnp.float32)[0:1]
            taken = (slot == position) & (member > 0.5)
            weighted = jnp.where(taken, weight, 0.0)
            top = weighted.astype(jnp.bfloat16)
            span = slice(h * cap, (h + 1) * cap)
            high[m, span, :] = top
            low[m, span, :] = (weighted - top.astype(jnp.float32)).astype(jnp.bfloat16)
            hot[h] = jnp.where(taken, 1.0, 0.0).astype(jnp.bfloat16)

    def project(u):
        i, h = lax.div(u, held), lax.rem(u, held)
        m = mask_of(i)

        @pl.when(h == 0)
        def _():
            @pl.when(i > 0)
            def _():
                info_direct(m).wait_recv()

                @pl.when(m != 6)
                def _():
                    tok_direct(m).wait_recv()

                @pl.when(m == 2)
                def _():
                    @pl.when(inner)
                    def _():
                        tok_relay(*relays[0]).start()
                        tok_direct(6).wait_recv()
                        tok_relay(*relays[1]).start()

                    tok_onward(2).start()

                @pl.when(m == 4)
                def _():
                    @pl.when(inner)
                    def _():
                        tok_relay(*relays[2]).start()

                    tok_onward(4).start()

                @pl.when(m == 5)
                def _():
                    @pl.when(jnp.logical_not(inner))
                    def _():
                        tok_direct(6).wait_recv()

                    tok_onward(6).start()

            slots_of(m)

        routed[...] = jnp.dot(
            hot[h], everyone[m], preferred_element_type=jnp.float32
        ).astype(jnp.bfloat16)

        @pl.when(u == 1)
        def _():
            load(0, 1).wait()
            load(1, 1).wait()
            load(2, 0).start()
            load(2, 1).start()

        for side in range(2):
            @pl.when(u == 0)
            def _():
                load_side(0, side).wait()
                load_side(1, side).wait()
                if side == 1:
                    load(0, 1).start()
                    load(1, 1).start()

            first = jnp.where(c == side, cols, 0)
            for which, w in enumerate((wg, wu)):
                for f in range(0, cols, TILE):
                    at = pl.multiple_of(first + f, 128)
                    got = jnp.dot(
                        routed[...], w[h, :, pl.ds(at, TILE)], preferred_element_type=jnp.float32
                    )
                    span = slice(which * cols + f, which * cols + f + TILE)
                    part[side, 0, :, span] = got[:half]
                    part[side, 1, :, span] = got[half:]
                if side == 0:
                    near_copy(u, which).start()

    def join(u):
        near_copy(u, 0).wait()
        near_copy(u, 1).wait()
        far_out[u] = (part[1, 1 - y] + near[u, 1 - y]).astype(jnp.bfloat16)
        far_copy(u).start()
        near[u, y] = near[u, y] + part[1, y]

    def activate(u):
        far_copy(u).wait()
        gate = near[u, y, :, :cols] + far_in[u, :, :cols].astype(jnp.float32)
        up = near[u, y, :, cols:] + far_in[u, :, cols:].astype(jnp.float32)
        hidden[u, c, y] = (gate / (1.0 + jnp.exp(-gate)) * up).astype(jnp.bfloat16)
        hidden_far(u).start()
        hidden_near(u).start()

    def relay(u):
        hidden_far(u).wait()
        hidden_onward(u).start()

    def finish(u):
        i, h = lax.div(u, held), lax.rem(u, held)
        m = mask_of(i)

        @pl.when(i == 0)
        def _():
            load(2, h).wait()

        hidden_near(u).wait()
        hidden_onward(u).wait()
        rows = jnp.concatenate([hidden[u, k].reshape(cap, cols) for k in range(2)], axis=1)
        for d in range(0, width, DOWN):
            rows_out[h, :, d:d + DOWN] = lax.dot_general(
                rows, wd[h, d:d + DOWN, :], (((1,), (1,)), ((), ())),
                preferred_element_type=jnp.float32,
            ).astype(jnp.bfloat16)

        @pl.when(h == held - 1)
        def _():
            both = rows_out[...].reshape(held * cap, width)
            over_slots = (((0,), (0,)), ((), ()))
            mixed = lax.dot_general(high[m], both, over_slots, preferred_element_type=jnp.float32)
            mixed = mixed + lax.dot_general(
                low[m], both, over_slots, preferred_element_type=jnp.float32
            )

            @pl.when(m == 0)
            def _():
                acc[...] = mixed

            @pl.when((m > 2) & (lax.rem(m, 2) == 0))
            def _():
                hold[lax.div(m, 2) - 2] = mixed

            @pl.when((lax.rem(m, 2) == 1) | (m == 2))
            def _():
                outgoing[m] = mixed.astype(jnp.bfloat16)
                ret_copy(m).start()

    def merge(u):
        m = jnp.where(u == 9, 4, 6)

        @pl.when((u == 9) | (u == 11))
        def _():
            ret_copy(m + 1).wait_recv()
            total = hold[lax.div(m, 2) - 2] + arrived[m + 1].astype(jnp.float32)
            outgoing[m] = total.astype(jnp.bfloat16)
            ret_copy(m).start()

    def early(u):
        @pl.when(u == units - 3)
        def _():
            finish(u)

    def late(u):
        @pl.when(u != units - 3)
        def _():
            finish(u)

    stages = (
        (1, join), (4, early), (2, activate), (0, project), (3, relay), (4, late), (4, merge),
    )

    def step(s, carry):
        for lag, stage in stages:
            @pl.when((s >= lag) & (s - lag < units))
            def _():
                stage(s - lag)
        return carry

    lax.fori_loop(0, units + 4, step, 0)

    def drain(m, carry):
        info_direct(m).wait_send()
        return carry

    lax.fori_loop(1, n_blk, drain, 0)
    for m in (1, 2):
        tok_direct(m).wait_send()
    for m in (2, 4, 6):
        tok_onward(m).wait_send()

    @pl.when(inner)
    def _():
        tok_middle().wait_send()
        for hop in relays:
            tok_relay(*hop).wait_send()

    for m in (2, 4, 6):
        ret_copy(m).wait_recv()
    acc[...] = acc[...] + sum(arrived[m].astype(jnp.float32) for m in (2, 4, 6))
    for m in (1, 2, 4, 5, 6, 7):
        ret_copy(m).wait_send()
    for m in (1, 3):
        ret_copy(m).wait_recv()
    out_ref[...] = (
        acc[...] + arrived[1].astype(jnp.float32) + arrived[3].astype(jnp.float32)
    ).astype(jnp.bfloat16)
    ret_copy(3).wait_send()


def fused(tokens, expert_ids, gate_vals, w_gate, w_up, w_down):
    n_blk = lax.axis_size("blk")
    tok_rows, width = tokens.shape
    held, _, ff = w_gate.shape
    capacity = 2 * tok_rows * expert_ids.shape[1] // (held * n_blk)
    half, units = capacity // 2, held * n_blk
    top_k = expert_ids.shape[1]
    lines = top_k + -top_k % 8
    bf, f32 = jnp.bfloat16, jnp.float32
    dma = pltpu.SemaphoreType.DMA
    counts = [n_blk + 1, n_blk, (2, 2), (2, 2)] + [RING] * 8 + [n_blk] * 4
    vmem = pl.BlockSpec(memory_space=pltpu.VMEM)
    anywhere = pl.BlockSpec(memory_space=pl.ANY)
    return pl.pallas_call(
        functools.partial(fused_kernel, n_blk),
        out_shape=pltpu.VMEM((tok_rows, width), bf),
        in_specs=[vmem] * 3 + [anywhere] * 3,
        out_specs=vmem,
        scratch_shapes=[
            pltpu.VMEM(w_gate.shape, bf),
            pltpu.VMEM(w_up.shape, bf),
            pltpu.VMEM(w_down.shape, bf),
            pltpu.VMEM((n_blk, tok_rows, width), bf),
            pltpu.VMEM((capacity, width), bf),
            pltpu.VMEM((2, 2, half, ff), f32),
            pltpu.VMEM((units, 2, half, ff), f32),
            pltpu.VMEM((units, half, ff), bf),
            pltpu.VMEM((units, half, ff), bf),
            pltpu.VMEM((units, 2, 2, half, ff // 2), bf),
            pltpu.VMEM((held, capacity, width), bf),
            pltpu.VMEM((n_blk, tok_rows, width), bf),
            pltpu.VMEM((n_blk, tok_rows, width), bf),
            pltpu.VMEM((n_blk // 2 - 2, tok_rows, width), f32),
            pltpu.VMEM((tok_rows, width), f32),
            pltpu.VMEM((n_blk, 2 * lines, tok_rows), f32),
            pltpu.VMEM((n_blk, held * capacity, tok_rows), bf),
            pltpu.VMEM((n_blk, held * capacity, tok_rows), bf),
            pltpu.VMEM((held, capacity, tok_rows), bf),
            dma((5, 2)),
        ] + [dma(count if isinstance(count, tuple) else (count,)) for count in counts],
        compiler_params=pltpu.CompilerParams(
            collective_id=0, has_side_effects=True, vmem_limit_bytes=VMEM_BYTES
        ),
    )(tokens, expert_ids.T, gate_vals.T, w_gate, w_up, w_down)


def routing(expert_ids, gate_vals, held_count, capacity):
    first = lax.axis_index("blk") * held_count
    top_k = expert_ids.shape[1]
    both = jnp.concatenate((expert_ids.astype(jnp.float32), gate_vals), axis=1)
    both = lax.all_gather(both, "blk", axis=0, tiled=False)
    ids, gates = both[:, :, :top_k].astype(jnp.int32), both[:, :, top_k:]
    mine = first + jnp.arange(held_count, dtype=jnp.int32)
    match = ids[:, None, :, :] == mine[None, :, None, None]
    member = jnp.any(match, axis=3)
    weight = jnp.sum(jnp.where(match, gates[:, None], 0.0), axis=3)
    tok_rows = ids.shape[1]
    earlier = jnp.triu(jnp.ones((tok_rows, tok_rows), jnp.float32), 1)
    position = jnp.einsum(
        "bht,tu->bhu", member.astype(jnp.bfloat16), earlier.astype(jnp.bfloat16),
        preferred_element_type=jnp.float32,
    )
    slots = jnp.arange(capacity, dtype=jnp.int32).astype(jnp.float32)
    hot = member[:, :, None, :] & (position[:, :, None, :] == slots[None, None, :, None])
    return hot.astype(jnp.bfloat16), jnp.where(hot, weight[:, :, None, :], 0.0)


def local(tokens, expert_ids, gate_vals, w_gate, w_up, w_down):
    blk_size = lax.axis_size("blk")
    tok_rows, width_dev = tokens.shape
    top_k = expert_ids.shape[1]
    held_count = w_gate.shape[0]
    capacity = 2 * tok_rows * top_k // (held_count * blk_size)
    hot, weighted = routing(expert_ids, gate_vals, held_count, capacity)
    everyone = lax.all_gather(tokens, "blk", axis=0, tiled=False)
    routed = jnp.einsum("bhpt,btd->hbpd", hot, everyone, preferred_element_type=jnp.float32)
    routed = routed.astype(jnp.bfloat16).reshape(held_count, blk_size * capacity, width_dev)
    gate_part = jnp.einsum("emd,edf->emf", routed, w_gate, preferred_element_type=jnp.float32)
    up_part = jnp.einsum("emd,edf->emf", routed, w_up, preferred_element_type=jnp.float32)
    both = jnp.stack((gate_part, up_part), axis=0)
    summed = lax.psum_scatter(both, "dp", scatter_dimension=2, tiled=True)
    hidden = (jax.nn.silu(summed[0]) * summed[1]).astype(jnp.bfloat16)
    hidden = lax.all_gather(hidden, "dp", axis=1, tiled=True)
    result = jnp.einsum("emf,edf->emd", hidden, w_down, preferred_element_type=jnp.float32)
    result = result.astype(jnp.bfloat16).reshape(held_count, blk_size, capacity, width_dev)
    high = weighted.astype(jnp.bfloat16)
    low = (weighted - high.astype(jnp.float32)).astype(jnp.bfloat16)
    partial = jnp.einsum(
        "bhpt,hbpd->btd", high, result, preferred_element_type=jnp.float32
    ) + jnp.einsum("bhpt,hbpd->btd", low, result, preferred_element_type=jnp.float32)
    partial = partial.astype(jnp.bfloat16).reshape(blk_size * tok_rows, width_dev)
    return lax.psum_scatter(partial, "blk", scatter_dimension=0, tiled=True)


def choose(tokens, expert_ids, gate_vals, w_gate, w_up, w_down):
    n_blk, held = lax.axis_size("blk"), w_gate.shape[0]
    capacity = 2 * tokens.shape[0] * expert_ids.shape[1] // (held * n_blk)
    fits = lax.axis_size("dp") == 4 and held == 2 and n_blk == 8 and capacity % 32 == 0
    fits = fits and w_gate.shape[2] % (2 * TILE) == 0 and tokens.shape[1] % DOWN == 0
    body = fused if fits else local
    return body(tokens, expert_ids, gate_vals, w_gate, w_up, w_down)


def solution(mesh):
    return jax.shard_map(
        choose,
        mesh=mesh,
        in_specs=(
            P("blk", "dp"),
            P("blk", None),
            P("blk", None),
            P("blk", "dp", None),
            P("blk", "dp", None),
            P("blk", "dp", None),
        ),
        out_specs=P("blk", "dp"),
        check_vma=False,
    )
```

```python
import functools

import jax
import jax.numpy as jnp
from jax import lax
from jax.experimental import pallas as pl
from jax.experimental.pallas import tpu as pltpu
from jax.sharding import PartitionSpec as P

MESH = pl.DeviceIdType.MESH
VMEM_BYTES = 66_000_000
TILE = 384
DOWN = 256
RING = 4
ORDER = (0, 2, 4, 5, 7, 6, 1, 3)


def flip(a, m, size):
    total, unit = 0, 1
    while unit < size:
        total = total + lax.rem(lax.div(a, unit) + lax.div(m, unit), 2) * unit
        unit *= 2
    return total


def fused_kernel(
    n_blk, tok_ref, ids_ref, gates_ref, wg_hbm, wu_hbm, wd_hbm, out_ref,
    wg, wu, wd, everyone, routed, part, near, far_out, far_in, hidden, rows_out,
    outgoing, arrived, hold, acc, info, high, low, hot,
    w_sem, tok_s, tok_r, near_s, near_r, far_s, far_r, hy_s, hy_r, hc_s, hc_r, hf_s, hf_r, ret_s, ret_r, info_s, info_r,
):
    blk = lax.axis_index("blk")
    dp = lax.axis_index("dp")
    y, c = lax.div(dp, 2), lax.rem(dp, 2)
    mate = (blk, y * 2 + (1 - c))
    across = (blk, (1 - y) * 2 + c)
    held, width, ff = wg.shape
    cols = ff // 2
    half = near.shape[2]
    cap = 2 * half
    units = held * n_blk

    def copy(src, dst, send, recv, device):
        return pltpu.make_async_remote_copy(
            src_ref=src, dst_ref=dst, send_sem=send, recv_sem=recv,
            device_id=device, device_id_type=MESH,
        )

    def peer(m):
        return (flip(blk, m, n_blk), dp)

    def mask_of(i):
        m = 0
        for k in range(1, n_blk):
            m = jnp.where(i == k, ORDER[k], m)
        return m

    def hop(m, k, to, have):
        tok, ids = (tok_ref, info.at[0]) if have is None else (everyone.at[have], info.at[have])
        return (
            copy(tok, everyone.at[m], tok_s.at[k], tok_r.at[m], peer(to)),
            copy(ids, info.at[m], info_s.at[k], info_r.at[m], peer(to)),
        )

    def send(hops):
        for part_of in hops:
            part_of.start()

    def sent(hops):
        for part_of in hops:
            part_of.wait_send()

    def received(m):
        for part_of in hop(m, m, m, None):
            part_of.wait_recv()

    def direct(m):
        return hop(m, m, m, None)

    def relay_hop(have, m, k, to):
        return hop(m, k, to, have)

    def onward(m):
        return hop(m + 1, m + 1, 1, m)

    def middle():
        return hop(6, 0, 6, None)

    relays = ((2, 4, 4, 6), (6, 4, 6, 2), (4, 6, n_blk, 2))

    def near_copy(u, which):
        k, span = lax.rem(u, 2), slice(which * cols, (which + 1) * cols)
        return copy(
            part.at[0, :, :, span], near.at[u, :, :, span], near_s.at[k, which], near_r.at[k, which], mate
        )

    def far_copy(u):
        return copy(far_out.at[u], far_in.at[u], far_s.at[lax.rem(u, RING)], far_r.at[lax.rem(u, RING)], across)

    def hidden_far(u):
        return copy(hidden.at[u, c, y], hidden.at[u, c, y], hy_s.at[lax.rem(u, RING)], hy_r.at[lax.rem(u, RING)], across)

    def hidden_near(u):
        return copy(hidden.at[u, c, y], hidden.at[u, c, y], hc_s.at[lax.rem(u, RING)], hc_r.at[lax.rem(u, RING)], mate)

    def hidden_onward(u):
        return copy(hidden.at[u, c, 1 - y], hidden.at[u, c, 1 - y], hf_s.at[lax.rem(u, RING)], hf_r.at[lax.rem(u, RING)], mate)

    def ret_copy(m):
        to = jnp.where((lax.rem(m, 2) == 1) & (m > 3), 1, m)
        return copy(outgoing.at[m], arrived.at[m], ret_s.at[m], ret_r.at[m], peer(to))

    def load(k, h):
        hbm, vmem = ((wg_hbm, wg), (wu_hbm, wu), (wd_hbm, wd))[k]
        return pltpu.make_async_copy(hbm.at[h], vmem.at[h], w_sem.at[k, h])

    def columns(side):
        return pl.multiple_of(jnp.where(c == side, cols, 0), 128)

    def load_side(k, side):
        hbm, vmem = ((wg_hbm, wg), (wu_hbm, wu))[k]
        span = (0, slice(None), pl.ds(columns(side), cols))
        return pltpu.make_async_copy(hbm.at[span], vmem.at[span], w_sem.at[3 + k, side])

    for side in range(2):
        for k in range(2):
            load_side(k, side).start()

    tok_rows = tok_ref.shape[0]
    top_k = ids_ref.shape[0]
    lines = info.shape[1] // 2
    inner = lax.rem(lax.div(lax.div(blk, 2) + 1, 2), 2) == 1
    info[0] = jnp.full(info.shape[1:], -1.0, jnp.float32)
    info[0, :top_k] = ids_ref[...].astype(jnp.float32)
    info[0, lines:lines + top_k] = gates_ref[...]

    barrier = pltpu.get_barrier_semaphore()
    for device in (peer(2), peer(1), mate, across):
        pl.semaphore_signal(barrier, inc=1, device_id=device, device_id_type=MESH)

    @pl.when(inner)
    def _():
        pl.semaphore_signal(barrier, inc=1, device_id=peer(6), device_id_type=MESH)

    pl.semaphore_wait(barrier, 4 + jnp.where(inner, 1, 0))

    send(direct(2))
    send(direct(1))

    @pl.when(inner)
    def _():
        send(middle())

    everyone[0] = tok_ref[...]

    def slots_of(m):
        square = (tok_rows, tok_rows)
        before = lax.broadcasted_iota(jnp.int32, square, 0) < lax.broadcasted_iota(jnp.int32, square, 1)
        before = jnp.where(before, 1.0, 0.0).astype(jnp.bfloat16)
        slot = lax.broadcasted_iota(jnp.int32, (cap, tok_rows), 0).astype(jnp.float32)
        ids, gates = info[m, :lines], info[m, lines:]
        for h in range(held):
            match = ids == (held * blk + h).astype(jnp.float32)
            member = jnp.sum(jnp.where(match, 1.0, 0.0), axis=0, keepdims=True)
            weight = jnp.sum(jnp.where(match, gates, 0.0), axis=0, keepdims=True)
            wide = jnp.broadcast_to(member, (16, tok_rows)).astype(jnp.bfloat16)
            position = jnp.dot(wide, before, preferred_element_type=jnp.float32)[0:1]
            taken = (slot == position) & (member > 0.5)
            weighted = jnp.where(taken, weight, 0.0)
            top = weighted.astype(jnp.bfloat16)
            span = slice(h * cap, (h + 1) * cap)
            high[m, span, :] = top
            low[m, span, :] = (weighted - top.astype(jnp.float32)).astype(jnp.bfloat16)
            hot[h] = jnp.where(taken, 1.0, 0.0).astype(jnp.bfloat16)

    def project(u):
        i, h = lax.div(u, held), lax.rem(u, held)
        m = mask_of(i)

        @pl.when(h == 0)
        def _():
            @pl.when(i > 0)
            def _():
                @pl.when(m != 6)
                def _():
                    received(m)

                @pl.when(m == 2)
                def _():
                    @pl.when(inner)
                    def _():
                        send(relay_hop(*relays[0]))
                        received(6)
                        send(relay_hop(*relays[1]))

                    send(onward(2))

                @pl.when(m == 4)
                def _():
                    @pl.when(inner)
                    def _():
                        send(relay_hop(*relays[2]))

                    send(onward(4))

                @pl.when(m == 5)
                def _():
                    @pl.when(jnp.logical_not(inner))
                    def _():
                        received(6)

                    send(onward(6))

            slots_of(m)

        routed[...] = jnp.dot(
            hot[h], everyone[m], preferred_element_type=jnp.float32
        ).astype(jnp.bfloat16)

        @pl.when(u == 1)
        def _():
            load(0, 1).wait()
            load(1, 1).wait()
            load(2, 0).start()
            load(2, 1).start()

        for side in range(2):
            @pl.when(u == 0)
            def _():
                load_side(0, side).wait()
                load_side(1, side).wait()
                if side == 0:
                    load(0, 1).start()
                    load(1, 1).start()

            first = jnp.where(c == side, cols, 0)
            for which, w in enumerate((wg, wu)):
                for f in range(0, cols, TILE):
                    at = pl.multiple_of(first + f, 128)
                    got = jnp.dot(
                        routed[...], w[h, :, pl.ds(at, TILE)], preferred_element_type=jnp.float32
                    )
                    span = slice(which * cols + f, which * cols + f + TILE)
                    part[side, 0, :, span] = got[:half]
                    part[side, 1, :, span] = got[half:]
                if side == 0:
                    near_copy(u, which).start()

    def join(u):
        near_copy(u, 0).wait()
        near_copy(u, 1).wait()
        far_out[u] = (part[1, 1 - y] + near[u, 1 - y]).astype(jnp.bfloat16)
        far_copy(u).start()
        near[u, y] = near[u, y] + part[1, y]

    def activate(u):
        far_copy(u).wait()
        gate = near[u, y, :, :cols] + far_in[u, :, :cols].astype(jnp.float32)
        up = near[u, y, :, cols:] + far_in[u, :, cols:].astype(jnp.float32)
        hidden[u, c, y] = (gate / (1.0 + jnp.exp(-gate)) * up).astype(jnp.bfloat16)
        hidden_far(u).start()
        hidden_near(u).start()

    def relay(u):
        hidden_far(u).wait()
        hidden_onward(u).start()

    def finish(u):
        i, h = lax.div(u, held), lax.rem(u, held)
        m = mask_of(i)

        @pl.when(i == 0)
        def _():
            load(2, h).wait()

        hidden_near(u).wait()
        hidden_onward(u).wait()
        rows = jnp.concatenate([hidden[u, k].reshape(cap, cols) for k in range(2)], axis=1)
        for d in range(0, width, DOWN):
            rows_out[h, :, d:d + DOWN] = lax.dot_general(
                rows, wd[h, d:d + DOWN, :], (((1,), (1,)), ((), ())),
                preferred_element_type=jnp.float32,
            ).astype(jnp.bfloat16)

        @pl.when(h == held - 1)
        def _():
            both = rows_out[...].reshape(held * cap, width)
            over_slots = (((0,), (0,)), ((), ()))
            mixed = lax.dot_general(high[m], both, over_slots, preferred_element_type=jnp.float32)
            mixed = mixed + lax.dot_general(
                low[m], both, over_slots, preferred_element_type=jnp.float32
            )

            @pl.when(m == 0)
            def _():
                acc[...] = mixed

            @pl.when((m > 2) & (lax.rem(m, 2) == 0))
            def _():
                hold[lax.div(m, 2) - 2] = mixed

            @pl.when((lax.rem(m, 2) == 1) | (m == 2))
            def _():
                outgoing[m] = mixed.astype(jnp.bfloat16)
                ret_copy(m).start()

    def merge(u):
        m = jnp.where(u == 9, 4, 6)

        @pl.when((u == 9) | (u == 11))
        def _():
            ret_copy(m + 1).wait_recv()
            total = hold[lax.div(m, 2) - 2] + arrived[m + 1].astype(jnp.float32)
            outgoing[m] = total.astype(jnp.bfloat16)
            ret_copy(m).start()

    def early(u):
        @pl.when(u == units - 3)
        def _():
            finish(u)

    def late(u):
        @pl.when(u != units - 3)
        def _():
            finish(u)

    stages = (
        (1, join), (4, early), (2, activate), (0, project), (3, relay), (4, late), (4, merge),
    )

    def step(s, carry):
        for lag, stage in stages:
            @pl.when((s >= lag) & (s - lag < units))
            def _():
                stage(s - lag)
        return carry

    lax.fori_loop(0, units + 4, step, 0)

    for m in (1, 2):
        sent(direct(m))
    for m in (2, 4, 6):
        sent(onward(m))

    @pl.when(inner)
    def _():
        sent(middle())
        for args in relays:
            sent(relay_hop(*args))

    for m in (2, 4, 6):
        ret_copy(m).wait_recv()
    acc[...] = acc[...] + sum(arrived[m].astype(jnp.float32) for m in (2, 4, 6))
    for m in (1, 2, 4, 5, 6, 7):
        ret_copy(m).wait_send()
    for m in (1, 3):
        ret_copy(m).wait_recv()
    out_ref[...] = (
        acc[...] + arrived[1].astype(jnp.float32) + arrived[3].astype(jnp.float32)
    ).astype(jnp.bfloat16)
    ret_copy(3).wait_send()


def fused(tokens, expert_ids, gate_vals, w_gate, w_up, w_down):
    n_blk = lax.axis_size("blk")
    tok_rows, width = tokens.shape
    held, _, ff = w_gate.shape
    capacity = 2 * tok_rows * expert_ids.shape[1] // (held * n_blk)
    half, units = capacity // 2, held * n_blk
    top_k = expert_ids.shape[1]
    lines = top_k + -top_k % 8
    bf, f32 = jnp.bfloat16, jnp.float32
    dma = pltpu.SemaphoreType.DMA
    counts = [n_blk + 1, n_blk, (2, 2), (2, 2)] + [RING] * 8 + [n_blk] * 2 + [n_blk + 1, n_blk]
    vmem = pl.BlockSpec(memory_space=pltpu.VMEM)
    anywhere = pl.BlockSpec(memory_space=pl.ANY)
    return pl.pallas_call(
        functools.partial(fused_kernel, n_blk),
        out_shape=pltpu.VMEM((tok_rows, width), bf),
        in_specs=[vmem] * 3 + [anywhere] * 3,
        out_specs=vmem,
        scratch_shapes=[
            pltpu.VMEM(w_gate.shape, bf),
            pltpu.VMEM(w_up.shape, bf),
            pltpu.VMEM(w_down.shape, bf),
            pltpu.VMEM((n_blk, tok_rows, width), bf),
            pltpu.VMEM((capacity, width), bf),
            pltpu.VMEM((2, 2, half, ff), f32),
            pltpu.VMEM((units, 2, half, ff), f32),
            pltpu.VMEM((units, half, ff), bf),
            pltpu.VMEM((units, half, ff), bf),
            pltpu.VMEM((units, 2, 2, half, ff // 2), bf),
            pltpu.VMEM((held, capacity, width), bf),
            pltpu.VMEM((n_blk, tok_rows, width), bf),
            pltpu.VMEM((n_blk, tok_rows, width), bf),
            pltpu.VMEM((n_blk // 2 - 2, tok_rows, width), f32),
            pltpu.VMEM((tok_rows, width), f32),
            pltpu.VMEM((n_blk, 2 * lines, tok_rows), f32),
            pltpu.VMEM((n_blk, held * capacity, tok_rows), bf),
            pltpu.VMEM((n_blk, held * capacity, tok_rows), bf),
            pltpu.VMEM((held, capacity, tok_rows), bf),
            dma((5, 2)),
        ] + [dma(count if isinstance(count, tuple) else (count,)) for count in counts],
        compiler_params=pltpu.CompilerParams(
            collective_id=0, has_side_effects=True, vmem_limit_bytes=VMEM_BYTES
        ),
    )(tokens, expert_ids.T, gate_vals.T, w_gate, w_up, w_down)


def routing(expert_ids, gate_vals, held_count, capacity):
    first = lax.axis_index("blk") * held_count
    top_k = expert_ids.shape[1]
    both = jnp.concatenate((expert_ids.astype(jnp.float32), gate_vals), axis=1)
    both = lax.all_gather(both, "blk", axis=0, tiled=False)
    ids, gates = both[:, :, :top_k].astype(jnp.int32), both[:, :, top_k:]
    mine = first + jnp.arange(held_count, dtype=jnp.int32)
    match = ids[:, None, :, :] == mine[None, :, None, None]
    member = jnp.any(match, axis=3)
    weight = jnp.sum(jnp.where(match, gates[:, None], 0.0), axis=3)
    tok_rows = ids.shape[1]
    earlier = jnp.triu(jnp.ones((tok_rows, tok_rows), jnp.float32), 1)
    position = jnp.einsum(
        "bht,tu->bhu", member.astype(jnp.bfloat16), earlier.astype(jnp.bfloat16),
        preferred_element_type=jnp.float32,
    )
    slots = jnp.arange(capacity, dtype=jnp.int32).astype(jnp.float32)
    hot = member[:, :, None, :] & (position[:, :, None, :] == slots[None, None, :, None])
    return hot.astype(jnp.bfloat16), jnp.where(hot, weight[:, :, None, :], 0.0)


def local(tokens, expert_ids, gate_vals, w_gate, w_up, w_down):
    blk_size = lax.axis_size("blk")
    tok_rows, width_dev = tokens.shape
    top_k = expert_ids.shape[1]
    held_count = w_gate.shape[0]
    capacity = 2 * tok_rows * top_k // (held_count * blk_size)
    hot, weighted = routing(expert_ids, gate_vals, held_count, capacity)
    everyone = lax.all_gather(tokens, "blk", axis=0, tiled=False)
    routed = jnp.einsum("bhpt,btd->hbpd", hot, everyone, preferred_element_type=jnp.float32)
    routed = routed.astype(jnp.bfloat16).reshape(held_count, blk_size * capacity, width_dev)
    gate_part = jnp.einsum("emd,edf->emf", routed, w_gate, preferred_element_type=jnp.float32)
    up_part = jnp.einsum("emd,edf->emf", routed, w_up, preferred_element_type=jnp.float32)
    both = jnp.stack((gate_part, up_part), axis=0)
    summed = lax.psum_scatter(both, "dp", scatter_dimension=2, tiled=True)
    hidden = (jax.nn.silu(summed[0]) * summed[1]).astype(jnp.bfloat16)
    hidden = lax.all_gather(hidden, "dp", axis=1, tiled=True)
    result = jnp.einsum("emf,edf->emd", hidden, w_down, preferred_element_type=jnp.float32)
    result = result.astype(jnp.bfloat16).reshape(held_count, blk_size, capacity, width_dev)
    high = weighted.astype(jnp.bfloat16)
    low = (weighted - high.astype(jnp.float32)).astype(jnp.bfloat16)
    partial = jnp.einsum(
        "bhpt,hbpd->btd", high, result, preferred_element_type=jnp.float32
    ) + jnp.einsum("bhpt,hbpd->btd", low, result, preferred_element_type=jnp.float32)
    partial = partial.astype(jnp.bfloat16).reshape(blk_size * tok_rows, width_dev)
    return lax.psum_scatter(partial, "blk", scatter_dimension=0, tiled=True)


def choose(tokens, expert_ids, gate_vals, w_gate, w_up, w_down):
    n_blk, held = lax.axis_size("blk"), w_gate.shape[0]
    capacity = 2 * tokens.shape[0] * expert_ids.shape[1] // (held * n_blk)
    fits = lax.axis_size("dp") == 4 and held == 2 and n_blk == 8 and capacity % 32 == 0
    fits = fits and w_gate.shape[2] % (2 * TILE) == 0 and tokens.shape[1] % DOWN == 0
    body = fused if fits else local
    return body(tokens, expert_ids, gate_vals, w_gate, w_up, w_down)


def solution(mesh):
    return jax.shard_map(
        choose,
        mesh=mesh,
        in_specs=(
            P("blk", "dp"),
            P("blk", None),
            P("blk", None),
            P("blk", "dp", None),
            P("blk", "dp", None),
            P("blk", "dp", None),
        ),
        out_specs=P("blk", "dp"),
        check_vma=False,
    )
```

```python
import functools

import jax
import jax.numpy as jnp
from jax import lax
from jax.experimental import pallas as pl
from jax.experimental.pallas import tpu as pltpu
from jax.sharding import PartitionSpec as P

MESH = pl.DeviceIdType.MESH
VMEM_BYTES = 66_000_000
TILE = 384
DOWN = 256
RING = 4
ORDER = (0, 2, 4, 5, 7, 6, 1, 3)


def flip(a, m, size):
    total, unit = 0, 1
    while unit < size:
        total = total + lax.rem(lax.div(a, unit) + lax.div(m, unit), 2) * unit
        unit *= 2
    return total


def fused_kernel(
    n_blk, tok_hbm, ids_hbm, gates_hbm, wg_hbm, wu_hbm, wd_hbm, out_ref,
    wg, wu, wd, everyone, routed, part, near, far_out, far_in, hidden, rows_out,
    outgoing, arrived, hold, acc, ids_ref, gates_ref, info, high, low, hot,
    w_sem, tok_s, tok_r, near_s, near_r, far_s, far_r, hy_s, hy_r, hc_s, hc_r, hf_s, hf_r, ret_s, ret_r, info_s, info_r,
):
    blk = lax.axis_index("blk")
    dp = lax.axis_index("dp")
    y, c = lax.div(dp, 2), lax.rem(dp, 2)
    mate = (blk, y * 2 + (1 - c))
    across = (blk, (1 - y) * 2 + c)
    held, width, ff = wg.shape
    cols = ff // 2
    half = near.shape[2]
    cap = 2 * half
    units = held * n_blk

    def copy(src, dst, send, recv, device):
        return pltpu.make_async_remote_copy(
            src_ref=src, dst_ref=dst, send_sem=send, recv_sem=recv,
            device_id=device, device_id_type=MESH,
        )

    def peer(m):
        return (flip(blk, m, n_blk), dp)

    def mask_of(i):
        m = 0
        for k in range(1, n_blk):
            m = jnp.where(i == k, ORDER[k], m)
        return m

    def hop(m, k, to, have):
        tok, ids = (everyone.at[have or 0], info.at[have or 0])
        return (
            copy(tok, everyone.at[m], tok_s.at[k], tok_r.at[m], peer(to)),
            copy(ids, info.at[m], info_s.at[k], info_r.at[m], peer(to)),
        )

    def send(hops):
        for part_of in hops:
            part_of.start()

    def sent(hops):
        for part_of in hops:
            part_of.wait_send()

    def received(m):
        for part_of in hop(m, m, m, None):
            part_of.wait_recv()

    def direct(m):
        return hop(m, m, m, None)

    def relay_hop(have, m, k, to):
        return hop(m, k, to, have)

    def onward(m):
        return hop(m + 1, m + 1, 1, m)

    def middle():
        return hop(6, 0, 6, None)

    relays = ((2, 4, 4, 6), (6, 4, 6, 2), (4, 6, n_blk, 2))

    def near_copy(u, which):
        k, span = lax.rem(u, 2), slice(which * cols, (which + 1) * cols)
        return copy(
            part.at[0, :, :, span], near.at[u, :, :, span], near_s.at[k, which], near_r.at[k, which], mate
        )

    def far_copy(u, which):
        k, span = lax.rem(u, RING), slice(which * cols, (which + 1) * cols)
        return copy(
            far_out.at[u, :, span], far_in.at[u, :, span], far_s.at[k, which], far_r.at[k, which], across
        )

    def hidden_far(u):
        return copy(hidden.at[u, c, y], hidden.at[u, c, y], hy_s.at[lax.rem(u, RING)], hy_r.at[lax.rem(u, RING)], across)

    def hidden_near(u):
        return copy(hidden.at[u, c, y], hidden.at[u, c, y], hc_s.at[lax.rem(u, RING)], hc_r.at[lax.rem(u, RING)], mate)

    def hidden_onward(u):
        return copy(hidden.at[u, c, 1 - y], hidden.at[u, c, 1 - y], hf_s.at[lax.rem(u, RING)], hf_r.at[lax.rem(u, RING)], mate)

    def ret_copy(m):
        to = jnp.where((lax.rem(m, 2) == 1) & (m > 3), 1, m)
        return copy(outgoing.at[m], arrived.at[m], ret_s.at[m], ret_r.at[m], peer(to))

    def load(k, h):
        hbm, vmem = ((wg_hbm, wg), (wu_hbm, wu), (wd_hbm, wd))[k]
        return pltpu.make_async_copy(hbm.at[h], vmem.at[h], w_sem.at[k, h])

    def columns(side):
        return pl.multiple_of(jnp.where(c == side, cols, 0), 128)

    def load_side(k, side):
        hbm, vmem = ((wg_hbm, wg), (wu_hbm, wu))[k]
        span = (0, slice(None), pl.ds(columns(side), cols))
        return pltpu.make_async_copy(hbm.at[span], vmem.at[span], w_sem.at[3 + k, side])

    inputs = [
        pltpu.make_async_copy(ids_hbm, ids_ref, w_sem.at[5, 0]),
        pltpu.make_async_copy(gates_hbm, gates_ref, w_sem.at[5, 1]),
        pltpu.make_async_copy(tok_hbm, everyone.at[0], w_sem.at[2, 0]),
    ]
    for load_in in inputs:
        load_in.start()
    for side in range(2):
        for k in range(2):
            load_side(k, side).start()

    inner = lax.rem(lax.div(lax.div(blk, 2) + 1, 2), 2) == 1
    barrier = pltpu.get_barrier_semaphore()
    for device in (peer(2), peer(1), mate, across):
        pl.semaphore_signal(barrier, inc=1, device_id=device, device_id_type=MESH)

    @pl.when(inner)
    def _():
        pl.semaphore_signal(barrier, inc=1, device_id=peer(6), device_id_type=MESH)

    tok_rows = everyone.shape[1]
    top_k = ids_ref.shape[0]
    lines = info.shape[1] // 2
    for load_in in inputs:
        load_in.wait()
    info[0] = jnp.full(info.shape[1:], -1.0, jnp.float32)
    info[0, :top_k] = ids_ref[...].astype(jnp.float32)
    info[0, lines:lines + top_k] = gates_ref[...]
    pl.semaphore_wait(barrier, 4 + jnp.where(inner, 1, 0))

    send(direct(2))
    send(direct(1))

    @pl.when(inner)
    def _():
        send(middle())


    def slots_of(m):
        square = (tok_rows, tok_rows)
        before = lax.broadcasted_iota(jnp.int32, square, 0) < lax.broadcasted_iota(jnp.int32, square, 1)
        before = jnp.where(before, 1.0, 0.0).astype(jnp.bfloat16)
        slot = lax.broadcasted_iota(jnp.int32, (cap, tok_rows), 0).astype(jnp.float32)
        ids, gates = info[m, :lines], info[m, lines:]
        for h in range(held):
            match = ids == (held * blk + h).astype(jnp.float32)
            member = jnp.sum(jnp.where(match, 1.0, 0.0), axis=0, keepdims=True)
            weight = jnp.sum(jnp.where(match, gates, 0.0), axis=0, keepdims=True)
            wide = jnp.broadcast_to(member, (16, tok_rows)).astype(jnp.bfloat16)
            position = jnp.dot(wide, before, preferred_element_type=jnp.float32)[0:1]
            taken = (slot == position) & (member > 0.5)
            weighted = jnp.where(taken, weight, 0.0)
            top = weighted.astype(jnp.bfloat16)
            span = slice(h * cap, (h + 1) * cap)
            high[m, span, :] = top
            low[m, span, :] = (weighted - top.astype(jnp.float32)).astype(jnp.bfloat16)
            hot[h] = jnp.where(taken, 1.0, 0.0).astype(jnp.bfloat16)

    def project(u):
        i, h = lax.div(u, held), lax.rem(u, held)
        m = mask_of(i)

        @pl.when(h == 0)
        def _():
            @pl.when(i > 0)
            def _():
                @pl.when(m != 6)
                def _():
                    received(m)

                @pl.when(m == 2)
                def _():
                    @pl.when(inner)
                    def _():
                        send(relay_hop(*relays[0]))
                        received(6)
                        send(relay_hop(*relays[1]))

                    send(onward(2))

                @pl.when(m == 4)
                def _():
                    @pl.when(inner)
                    def _():
                        send(relay_hop(*relays[2]))

                    send(onward(4))

                @pl.when(m == 5)
                def _():
                    @pl.when(jnp.logical_not(inner))
                    def _():
                        received(6)

                    send(onward(6))

            slots_of(m)

        routed[...] = jnp.dot(
            hot[h], everyone[m], preferred_element_type=jnp.float32
        ).astype(jnp.bfloat16)

        @pl.when(u == 1)
        def _():
            load(0, 1).wait()
            load(1, 1).wait()
            load(2, 0).start()
            load(2, 1).start()

        for side in range(2):
            @pl.when(u == 0)
            def _():
                load_side(0, side).wait()
                load_side(1, side).wait()
                if side == 0:
                    load(0, 1).start()
                    load(1, 1).start()

            first = jnp.where(c == side, cols, 0)
            for which, w in enumerate((wg, wu)):
                for f in range(0, cols, TILE):
                    at = pl.multiple_of(first + f, 128)
                    got = jnp.dot(
                        routed[...], w[h, :, pl.ds(at, TILE)], preferred_element_type=jnp.float32
                    )
                    span = slice(which * cols + f, which * cols + f + TILE)
                    part[side, 0, :, span] = got[:half]
                    part[side, 1, :, span] = got[half:]
                if side == 0:
                    near_copy(u, which).start()

    def join(u):
        for which in range(2):
            span = slice(which * cols, (which + 1) * cols)
            near_copy(u, which).wait()
            far_out[u, :, span] = (part[1, 1 - y, :, span] + near[u, 1 - y, :, span]).astype(jnp.bfloat16)
            far_copy(u, which).start()
        near[u, y] = near[u, y] + part[1, y]

    def activate(u):
        far_copy(u, 0).wait()
        far_copy(u, 1).wait()
        gate = near[u, y, :, :cols] + far_in[u, :, :cols].astype(jnp.float32)
        up = near[u, y, :, cols:] + far_in[u, :, cols:].astype(jnp.float32)
        hidden[u, c, y] = (gate / (1.0 + jnp.exp(-gate)) * up).astype(jnp.bfloat16)
        hidden_far(u).start()
        hidden_near(u).start()

    def relay(u):
        hidden_far(u).wait()
        hidden_onward(u).start()

    def finish(u):
        i, h = lax.div(u, held), lax.rem(u, held)
        m = mask_of(i)

        @pl.when(i == 0)
        def _():
            load(2, h).wait()

        hidden_near(u).wait()
        hidden_onward(u).wait()
        rows = jnp.concatenate([hidden[u, k].reshape(cap, cols) for k in range(2)], axis=1)
        for d in range(0, width, DOWN):
            rows_out[h, :, d:d + DOWN] = lax.dot_general(
                rows, wd[h, d:d + DOWN, :], (((1,), (1,)), ((), ())),
                preferred_element_type=jnp.float32,
            ).astype(jnp.bfloat16)

        @pl.when(h == held - 1)
        def _():
            both = rows_out[...].reshape(held * cap, width)
            over_slots = (((0,), (0,)), ((), ()))
            mixed = lax.dot_general(high[m], both, over_slots, preferred_element_type=jnp.float32)
            mixed = mixed + lax.dot_general(
                low[m], both, over_slots, preferred_element_type=jnp.float32
            )

            @pl.when(m == 0)
            def _():
                acc[...] = mixed

            @pl.when((m > 2) & (lax.rem(m, 2) == 0))
            def _():
                hold[lax.div(m, 2) - 2] = mixed

            @pl.when((lax.rem(m, 2) == 1) | (m == 2))
            def _():
                outgoing[m] = mixed.astype(jnp.bfloat16)
                ret_copy(m).start()

    def merge(u):
        m = jnp.where(u == 9, 4, 6)

        @pl.when((u == 9) | (u == 11))
        def _():
            ret_copy(m + 1).wait_recv()
            total = hold[lax.div(m, 2) - 2] + arrived[m + 1].astype(jnp.float32)
            outgoing[m] = total.astype(jnp.bfloat16)
            ret_copy(m).start()

    def early(u):
        @pl.when(u == units - 3)
        def _():
            finish(u)

    def late(u):
        @pl.when(u != units - 3)
        def _():
            finish(u)

    stages = (
        (1, join), (4, early), (2, activate), (0, project), (3, relay), (4, late), (4, merge),
    )

    def step(s, carry):
        for lag, stage in stages:
            @pl.when((s >= lag) & (s - lag < units))
            def _():
                stage(s - lag)
        return carry

    lax.fori_loop(0, units + 4, step, 0)

    for m in (1, 2):
        sent(direct(m))
    for m in (2, 4, 6):
        sent(onward(m))

    @pl.when(inner)
    def _():
        sent(middle())
        for args in relays:
            sent(relay_hop(*args))

    for m in (2, 4, 6):
        ret_copy(m).wait_recv()
    acc[...] = acc[...] + sum(arrived[m].astype(jnp.float32) for m in (2, 4, 6))
    for m in (1, 2, 4, 5, 6, 7):
        ret_copy(m).wait_send()
    ret_copy(1).wait_recv()
    acc[...] = acc[...] + arrived[1].astype(jnp.float32)
    ret_copy(3).wait_recv()
    out_ref[...] = (acc[...] + arrived[3].astype(jnp.float32)).astype(jnp.bfloat16)
    ret_copy(3).wait_send()


def fused(tokens, expert_ids, gate_vals, w_gate, w_up, w_down):
    n_blk = lax.axis_size("blk")
    tok_rows, width = tokens.shape
    held, _, ff = w_gate.shape
    capacity = 2 * tok_rows * expert_ids.shape[1] // (held * n_blk)
    half, units = capacity // 2, held * n_blk
    top_k = expert_ids.shape[1]
    lines = top_k + -top_k % 8
    bf, f32 = jnp.bfloat16, jnp.float32
    dma = pltpu.SemaphoreType.DMA
    counts = [n_blk + 1, n_blk, (2, 2), (2, 2)] + [(RING, 2)] * 2 + [RING] * 6 + [n_blk] * 2 + [n_blk + 1, n_blk]
    vmem = pl.BlockSpec(memory_space=pltpu.VMEM)
    anywhere = pl.BlockSpec(memory_space=pl.ANY)
    return pl.pallas_call(
        functools.partial(fused_kernel, n_blk),
        out_shape=pltpu.VMEM((tok_rows, width), bf),
        in_specs=[anywhere] * 6,
        out_specs=vmem,
        scratch_shapes=[
            pltpu.VMEM(w_gate.shape, bf),
            pltpu.VMEM(w_up.shape, bf),
            pltpu.VMEM(w_down.shape, bf),
            pltpu.VMEM((n_blk, tok_rows, width), bf),
            pltpu.VMEM((capacity, width), bf),
            pltpu.VMEM((2, 2, half, ff), f32),
            pltpu.VMEM((units, 2, half, ff), f32),
            pltpu.VMEM((units, half, ff), bf),
            pltpu.VMEM((units, half, ff), bf),
            pltpu.VMEM((units, 2, 2, half, ff // 2), bf),
            pltpu.VMEM((held, capacity, width), bf),
            pltpu.VMEM((n_blk, tok_rows, width), bf),
            pltpu.VMEM((n_blk, tok_rows, width), bf),
            pltpu.VMEM((n_blk // 2 - 2, tok_rows, width), f32),
            pltpu.VMEM((tok_rows, width), f32),
            pltpu.VMEM((top_k, tok_rows), jnp.int32),
            pltpu.VMEM((top_k, tok_rows), f32),
            pltpu.VMEM((n_blk, 2 * lines, tok_rows), f32),
            pltpu.VMEM((n_blk, held * capacity, tok_rows), bf),
            pltpu.VMEM((n_blk, held * capacity, tok_rows), bf),
            pltpu.VMEM((held, capacity, tok_rows), bf),
            dma((6, 2)),
        ] + [dma(count if isinstance(count, tuple) else (count,)) for count in counts],
        compiler_params=pltpu.CompilerParams(
            collective_id=0, has_side_effects=True, vmem_limit_bytes=VMEM_BYTES
        ),
    )(tokens, expert_ids.T, gate_vals.T, w_gate, w_up, w_down)


def routing(expert_ids, gate_vals, held_count, capacity):
    first = lax.axis_index("blk") * held_count
    top_k = expert_ids.shape[1]
    both = jnp.concatenate((expert_ids.astype(jnp.float32), gate_vals), axis=1)
    both = lax.all_gather(both, "blk", axis=0, tiled=False)
    ids, gates = both[:, :, :top_k].astype(jnp.int32), both[:, :, top_k:]
    mine = first + jnp.arange(held_count, dtype=jnp.int32)
    match = ids[:, None, :, :] == mine[None, :, None, None]
    member = jnp.any(match, axis=3)
    weight = jnp.sum(jnp.where(match, gates[:, None], 0.0), axis=3)
    tok_rows = ids.shape[1]
    earlier = jnp.triu(jnp.ones((tok_rows, tok_rows), jnp.float32), 1)
    position = jnp.einsum(
        "bht,tu->bhu", member.astype(jnp.bfloat16), earlier.astype(jnp.bfloat16),
        preferred_element_type=jnp.float32,
    )
    slots = jnp.arange(capacity, dtype=jnp.int32).astype(jnp.float32)
    hot = member[:, :, None, :] & (position[:, :, None, :] == slots[None, None, :, None])
    return hot.astype(jnp.bfloat16), jnp.where(hot, weight[:, :, None, :], 0.0)


def local(tokens, expert_ids, gate_vals, w_gate, w_up, w_down):
    blk_size = lax.axis_size("blk")
    tok_rows, width_dev = tokens.shape
    top_k = expert_ids.shape[1]
    held_count = w_gate.shape[0]
    capacity = 2 * tok_rows * top_k // (held_count * blk_size)
    hot, weighted = routing(expert_ids, gate_vals, held_count, capacity)
    everyone = lax.all_gather(tokens, "blk", axis=0, tiled=False)
    routed = jnp.einsum("bhpt,btd->hbpd", hot, everyone, preferred_element_type=jnp.float32)
    routed = routed.astype(jnp.bfloat16).reshape(held_count, blk_size * capacity, width_dev)
    gate_part = jnp.einsum("emd,edf->emf", routed, w_gate, preferred_element_type=jnp.float32)
    up_part = jnp.einsum("emd,edf->emf", routed, w_up, preferred_element_type=jnp.float32)
    both = jnp.stack((gate_part, up_part), axis=0)
    summed = lax.psum_scatter(both, "dp", scatter_dimension=2, tiled=True)
    hidden = (jax.nn.silu(summed[0]) * summed[1]).astype(jnp.bfloat16)
    hidden = lax.all_gather(hidden, "dp", axis=1, tiled=True)
    result = jnp.einsum("emf,edf->emd", hidden, w_down, preferred_element_type=jnp.float32)
    result = result.astype(jnp.bfloat16).reshape(held_count, blk_size, capacity, width_dev)
    high = weighted.astype(jnp.bfloat16)
    low = (weighted - high.astype(jnp.float32)).astype(jnp.bfloat16)
    partial = jnp.einsum(
        "bhpt,hbpd->btd", high, result, preferred_element_type=jnp.float32
    ) + jnp.einsum("bhpt,hbpd->btd", low, result, preferred_element_type=jnp.float32)
    partial = partial.astype(jnp.bfloat16).reshape(blk_size * tok_rows, width_dev)
    return lax.psum_scatter(partial, "blk", scatter_dimension=0, tiled=True)


def choose(tokens, expert_ids, gate_vals, w_gate, w_up, w_down):
    n_blk, held = lax.axis_size("blk"), w_gate.shape[0]
    capacity = 2 * tokens.shape[0] * expert_ids.shape[1] // (held * n_blk)
    fits = lax.axis_size("dp") == 4 and held == 2 and n_blk == 8 and capacity % 32 == 0
    fits = fits and w_gate.shape[2] % (2 * TILE) == 0 and tokens.shape[1] % DOWN == 0
    body = fused if fits else local
    return body(tokens, expert_ids, gate_vals, w_gate, w_up, w_down)


def solution(mesh):
    return jax.shard_map(
        choose,
        mesh=mesh,
        in_specs=(
            P("blk", "dp"),
            P("blk", None),
            P("blk", None),
            P("blk", "dp", None),
            P("blk", "dp", None),
            P("blk", "dp", None),
        ),
        out_specs=P("blk", "dp"),
        check_vma=False,
    )
```

```python
import functools

import jax
import jax.numpy as jnp
from jax import lax
from jax.experimental import pallas as pl
from jax.experimental.pallas import tpu as pltpu
from jax.sharding import PartitionSpec as P

MESH = pl.DeviceIdType.MESH
VMEM_BYTES = 66_000_000
TILE = 384
DOWN = 256
RING = 4
SPLIT = 512
ORDER = (0, 2, 4, 5, 7, 6, 1, 3)


def flip(a, m, size):
    total, unit = 0, 1
    while unit < size:
        total = total + lax.rem(lax.div(a, unit) + lax.div(m, unit), 2) * unit
        unit *= 2
    return total


def fused_kernel(
    n_blk, tok_hbm, ids_hbm, gates_hbm, wg_hbm, wu_hbm, wd_hbm, out_ref,
    wg, wu, wd, everyone, routed, part, near, far_out, far_in, hidden, rows_out,
    outgoing, arrived, hold, acc, ids_ref, gates_ref, info, high, low, hot,
    w_sem, tok_s, tok_r, near_s, near_r, far_s, far_r, hy_s, hy_r, hc_s, hc_r, hf_s, hf_r, ret_s, ret_r, info_s, info_r,
):
    blk = lax.axis_index("blk")
    dp = lax.axis_index("dp")
    y, c = lax.div(dp, 2), lax.rem(dp, 2)
    mate = (blk, y * 2 + (1 - c))
    across = (blk, (1 - y) * 2 + c)
    held, width, ff = wg.shape
    cols = ff // 2
    half = near.shape[2]
    cap = 2 * half
    units = held * n_blk

    def copy(src, dst, send, recv, device):
        return pltpu.make_async_remote_copy(
            src_ref=src, dst_ref=dst, send_sem=send, recv_sem=recv,
            device_id=device, device_id_type=MESH,
        )

    def peer(m):
        return (flip(blk, m, n_blk), dp)

    def mask_of(i):
        m = 0
        for k in range(1, n_blk):
            m = jnp.where(i == k, ORDER[k], m)
        return m

    def hop(m, k, to, have):
        tok, ids = (everyone.at[have or 0], info.at[have or 0])
        return (
            copy(tok, everyone.at[m], tok_s.at[k], tok_r.at[m], peer(to)),
            copy(ids, info.at[m], info_s.at[k], info_r.at[m], peer(to)),
        )

    def send(hops):
        for part_of in hops:
            part_of.start()

    def sent(hops):
        for part_of in hops:
            part_of.wait_send()

    def received(m):
        for part_of in hop(m, m, m, None):
            part_of.wait_recv()

    def direct(m):
        return hop(m, m, m, None)

    def relay_hop(have, m, k, to):
        return hop(m, k, to, have)

    def onward(m):
        return hop(m + 1, m + 1, 1, m)

    def middle():
        return hop(6, 0, 6, None)

    relays = ((2, 4, 4, 6), (6, 4, 6, 2), (4, 6, n_blk, 2))

    def near_copy(u, which):
        k, span = lax.rem(u, 2), slice(which * cols, (which + 1) * cols)
        return copy(
            part.at[0, :, :, span], near.at[u, :, :, span], near_s.at[k, which], near_r.at[k, which], mate
        )

    def far_copy(u, which):
        k, span = lax.rem(u, RING), slice(which * cols, (which + 1) * cols)
        return copy(
            far_out.at[u, :, span], far_in.at[u, :, span], far_s.at[k, which], far_r.at[k, which], across
        )

    def hidden_far(u):
        return copy(hidden.at[u, c, y], hidden.at[u, c, y], hy_s.at[lax.rem(u, RING)], hy_r.at[lax.rem(u, RING)], across)

    def hidden_near(u):
        return copy(hidden.at[u, c, y], hidden.at[u, c, y], hc_s.at[lax.rem(u, RING)], hc_r.at[lax.rem(u, RING)], mate)

    def hidden_onward(u):
        return copy(hidden.at[u, c, 1 - y], hidden.at[u, c, 1 - y], hf_s.at[lax.rem(u, RING)], hf_r.at[lax.rem(u, RING)], mate)

    def ret_copy(m):
        to = jnp.where((lax.rem(m, 2) == 1) & (m > 3), 1, m)
        return copy(outgoing.at[m], arrived.at[m], ret_s.at[m], ret_r.at[m], peer(to))

    spans = ((0, SPLIT), (SPLIT, width))

    def ret_part(m, k):
        d0, d1 = spans[k]
        sem = m if k == 0 else jnp.where(m == 1, 0, n_blk)
        return copy(
            outgoing.at[m, :, d0:d1], arrived.at[m, :, d0:d1], ret_s.at[sem], ret_r.at[sem], peer(m)
        )

    def load(k, h):
        hbm, vmem = ((wg_hbm, wg), (wu_hbm, wu), (wd_hbm, wd))[k]
        return pltpu.make_async_copy(hbm.at[h], vmem.at[h], w_sem.at[k, h])

    def columns(side):
        return pl.multiple_of(jnp.where(c == side, cols, 0), 128)

    def load_side(k, side):
        hbm, vmem = ((wg_hbm, wg), (wu_hbm, wu))[k]
        span = (0, slice(None), pl.ds(columns(side), cols))
        return pltpu.make_async_copy(hbm.at[span], vmem.at[span], w_sem.at[3 + k, side])

    inputs = [
        pltpu.make_async_copy(ids_hbm, ids_ref, w_sem.at[5, 0]),
        pltpu.make_async_copy(gates_hbm, gates_ref, w_sem.at[5, 1]),
        pltpu.make_async_copy(tok_hbm, everyone.at[0], w_sem.at[2, 0]),
    ]
    for load_in in inputs:
        load_in.start()
    for side in range(2):
        for k in range(2):
            load_side(k, side).start()

    inner = lax.rem(lax.div(lax.div(blk, 2) + 1, 2), 2) == 1
    barrier = pltpu.get_barrier_semaphore()
    for device in (peer(2), peer(1), mate, across):
        pl.semaphore_signal(barrier, inc=1, device_id=device, device_id_type=MESH)

    @pl.when(inner)
    def _():
        pl.semaphore_signal(barrier, inc=1, device_id=peer(6), device_id_type=MESH)

    tok_rows = everyone.shape[1]
    top_k = ids_ref.shape[0]
    lines = info.shape[1] // 2
    for load_in in inputs:
        load_in.wait()
    info[0] = jnp.full(info.shape[1:], -1.0, jnp.float32)
    info[0, :top_k] = ids_ref[...].astype(jnp.float32)
    info[0, lines:lines + top_k] = gates_ref[...]
    pl.semaphore_wait(barrier, 4 + jnp.where(inner, 1, 0))

    send(direct(2))
    send(direct(1))

    @pl.when(inner)
    def _():
        send(middle())


    def slots_of(m):
        square = (tok_rows, tok_rows)
        before = lax.broadcasted_iota(jnp.int32, square, 0) < lax.broadcasted_iota(jnp.int32, square, 1)
        before = jnp.where(before, 1.0, 0.0).astype(jnp.bfloat16)
        slot = lax.broadcasted_iota(jnp.int32, (cap, tok_rows), 0).astype(jnp.float32)
        ids, gates = info[m, :lines], info[m, lines:]
        for h in range(held):
            match = ids == (held * blk + h).astype(jnp.float32)
            member = jnp.sum(jnp.where(match, 1.0, 0.0), axis=0, keepdims=True)
            weight = jnp.sum(jnp.where(match, gates, 0.0), axis=0, keepdims=True)
            wide = jnp.broadcast_to(member, (16, tok_rows)).astype(jnp.bfloat16)
            position = jnp.dot(wide, before, preferred_element_type=jnp.float32)[0:1]
            taken = (slot == position) & (member > 0.5)
            weighted = jnp.where(taken, weight, 0.0)
            top = weighted.astype(jnp.bfloat16)
            span = slice(h * cap, (h + 1) * cap)
            high[m, span, :] = top
            low[m, span, :] = (weighted - top.astype(jnp.float32)).astype(jnp.bfloat16)
            hot[h] = jnp.where(taken, 1.0, 0.0).astype(jnp.bfloat16)

    def project(u):
        i, h = lax.div(u, held), lax.rem(u, held)
        m = mask_of(i)

        @pl.when(h == 0)
        def _():
            @pl.when(i > 0)
            def _():
                @pl.when(m != 6)
                def _():
                    received(m)

                @pl.when(m == 2)
                def _():
                    @pl.when(inner)
                    def _():
                        send(relay_hop(*relays[0]))
                        received(6)
                        send(relay_hop(*relays[1]))

                    send(onward(2))

                @pl.when(m == 4)
                def _():
                    @pl.when(inner)
                    def _():
                        send(relay_hop(*relays[2]))

                    send(onward(4))

                @pl.when(m == 5)
                def _():
                    @pl.when(jnp.logical_not(inner))
                    def _():
                        received(6)

                    send(onward(6))

            slots_of(m)

        routed[...] = jnp.dot(
            hot[h], everyone[m], preferred_element_type=jnp.float32
        ).astype(jnp.bfloat16)

        @pl.when(u == 1)
        def _():
            load(0, 1).wait()
            load(1, 1).wait()
            load(2, 0).start()
            load(2, 1).start()

        for side in range(2):
            first = jnp.where(c == side, cols, 0)
            for which, w in enumerate((wg, wu)):
                @pl.when(u == 0)
                def _():
                    load_side(which, side).wait()
                    if side == 0 and which == 1:
                        load(0, 1).start()
                        load(1, 1).start()

                for f in range(0, cols, TILE):
                    at = pl.multiple_of(first + f, 128)
                    got = jnp.dot(
                        routed[...], w[h, :, pl.ds(at, TILE)], preferred_element_type=jnp.float32
                    )
                    span = slice(which * cols + f, which * cols + f + TILE)
                    part[side, 0, :, span] = got[:half]
                    part[side, 1, :, span] = got[half:]
                if side == 0:
                    near_copy(u, which).start()

    def join(u):
        for which in range(2):
            span = slice(which * cols, (which + 1) * cols)
            near_copy(u, which).wait()
            far_out[u, :, span] = (part[1, 1 - y, :, span] + near[u, 1 - y, :, span]).astype(jnp.bfloat16)
            far_copy(u, which).start()
        near[u, y] = near[u, y] + part[1, y]

    def activate(u):
        far_copy(u, 0).wait()
        far_copy(u, 1).wait()
        gate = near[u, y, :, :cols] + far_in[u, :, :cols].astype(jnp.float32)
        up = near[u, y, :, cols:] + far_in[u, :, cols:].astype(jnp.float32)
        hidden[u, c, y] = (gate / (1.0 + jnp.exp(-gate)) * up).astype(jnp.bfloat16)
        hidden_far(u).start()
        hidden_near(u).start()

    def relay(u):
        hidden_far(u).wait()
        hidden_onward(u).start()

    def finish(u):
        i, h = lax.div(u, held), lax.rem(u, held)
        m = mask_of(i)

        @pl.when(i == 0)
        def _():
            load(2, h).wait()

        hidden_near(u).wait()
        hidden_onward(u).wait()
        rows = jnp.concatenate([hidden[u, k].reshape(cap, cols) for k in range(2)], axis=1)
        def down(d0, d1):
            for d in range(d0, d1, DOWN):
                rows_out[h, :, d:d + DOWN] = lax.dot_general(
                    rows, wd[h, d:d + DOWN, :], (((1,), (1,)), ((), ())),
                    preferred_element_type=jnp.float32,
                ).astype(jnp.bfloat16)

        def mix(d0, d1):
            both = rows_out[:, :, d0:d1].reshape(held * cap, d1 - d0)
            over_slots = (((0,), (0,)), ((), ()))
            mixed = lax.dot_general(high[m], both, over_slots, preferred_element_type=jnp.float32)
            return mixed + lax.dot_general(
                low[m], both, over_slots, preferred_element_type=jnp.float32
            )

        last = (m == 1) | (m == 3)

        @pl.when((h < held - 1) | jnp.logical_not(last))
        def _():
            down(0, width)

        @pl.when((h == held - 1) & last)
        def _():
            for k, (d0, d1) in enumerate(spans):
                down(d0, d1)
                outgoing[m, :, d0:d1] = mix(d0, d1).astype(jnp.bfloat16)
                ret_part(m, k).start()

        @pl.when((h == held - 1) & jnp.logical_not(last))
        def _():
            mixed = mix(0, width)

            @pl.when(m == 0)
            def _():
                acc[...] = mixed

            @pl.when((m > 2) & (lax.rem(m, 2) == 0))
            def _():
                hold[lax.div(m, 2) - 2] = mixed

            @pl.when((lax.rem(m, 2) == 1) | (m == 2))
            def _():
                outgoing[m] = mixed.astype(jnp.bfloat16)
                ret_copy(m).start()

    def merge(u):
        m = jnp.where(u == 9, 4, 6)

        @pl.when((u == 9) | (u == 11))
        def _():
            ret_copy(m + 1).wait_recv()
            total = hold[lax.div(m, 2) - 2] + arrived[m + 1].astype(jnp.float32)
            outgoing[m] = total.astype(jnp.bfloat16)
            ret_copy(m).start()

    def early(u):
        @pl.when(u == units - 3)
        def _():
            finish(u)

    def late(u):
        @pl.when(u != units - 3)
        def _():
            finish(u)

    stages = (
        (1, join), (4, early), (2, activate), (0, project), (3, relay), (4, late), (4, merge),
    )

    def step(s, carry):
        for lag, stage in stages:
            @pl.when((s >= lag) & (s - lag < units))
            def _():
                stage(s - lag)
        return carry

    lax.fori_loop(0, units + 4, step, 0)

    for m in (1, 2):
        sent(direct(m))
    for m in (2, 4, 6):
        sent(onward(m))

    @pl.when(inner)
    def _():
        sent(middle())
        for args in relays:
            sent(relay_hop(*args))

    for m in (2, 4, 6):
        ret_copy(m).wait_recv()
    acc[...] = acc[...] + sum(arrived[m].astype(jnp.float32) for m in (2, 4, 6))
    for m in (2, 4, 5, 6, 7):
        ret_copy(m).wait_send()
    for k in range(2):
        ret_part(1, k).wait_send()
    for k in range(2):
        ret_part(1, k).wait_recv()
    acc[...] = acc[...] + arrived[1].astype(jnp.float32)
    for k, (d0, d1) in enumerate(spans):
        ret_part(3, k).wait_recv()
        out_ref[:, d0:d1] = (acc[:, d0:d1] + arrived[3, :, d0:d1].astype(jnp.float32)).astype(jnp.bfloat16)
    for k in range(2):
        ret_part(3, k).wait_send()


def fused(tokens, expert_ids, gate_vals, w_gate, w_up, w_down):
    n_blk = lax.axis_size("blk")
    tok_rows, width = tokens.shape
    held, _, ff = w_gate.shape
    capacity = 2 * tok_rows * expert_ids.shape[1] // (held * n_blk)
    half, units = capacity // 2, held * n_blk
    top_k = expert_ids.shape[1]
    lines = top_k + -top_k % 8
    bf, f32 = jnp.bfloat16, jnp.float32
    dma = pltpu.SemaphoreType.DMA
    counts = [n_blk + 1, n_blk, (2, 2), (2, 2)] + [(RING, 2)] * 2 + [RING] * 6 + [n_blk + 1] * 3 + [n_blk]
    vmem = pl.BlockSpec(memory_space=pltpu.VMEM)
    anywhere = pl.BlockSpec(memory_space=pl.ANY)
    return pl.pallas_call(
        functools.partial(fused_kernel, n_blk),
        out_shape=pltpu.VMEM((tok_rows, width), bf),
        in_specs=[anywhere] * 6,
        out_specs=vmem,
        scratch_shapes=[
            pltpu.VMEM(w_gate.shape, bf),
            pltpu.VMEM(w_up.shape, bf),
            pltpu.VMEM(w_down.shape, bf),
            pltpu.VMEM((n_blk, tok_rows, width), bf),
            pltpu.VMEM((capacity, width), bf),
            pltpu.VMEM((2, 2, half, ff), f32),
            pltpu.VMEM((units, 2, half, ff), f32),
            pltpu.VMEM((units, half, ff), bf),
            pltpu.VMEM((units, half, ff), bf),
            pltpu.VMEM((units, 2, 2, half, ff // 2), bf),
            pltpu.VMEM((held, capacity, width), bf),
            pltpu.VMEM((n_blk, tok_rows, width), bf),
            pltpu.VMEM((n_blk, tok_rows, width), bf),
            pltpu.VMEM((n_blk // 2 - 2, tok_rows, width), f32),
            pltpu.VMEM((tok_rows, width), f32),
            pltpu.VMEM((top_k, tok_rows), jnp.int32),
            pltpu.VMEM((top_k, tok_rows), f32),
            pltpu.VMEM((n_blk, 2 * lines, tok_rows), f32),
            pltpu.VMEM((n_blk, held * capacity, tok_rows), bf),
            pltpu.VMEM((n_blk, held * capacity, tok_rows), bf),
            pltpu.VMEM((held, capacity, tok_rows), bf),
            dma((6, 2)),
        ] + [dma(count if isinstance(count, tuple) else (count,)) for count in counts],
        compiler_params=pltpu.CompilerParams(
            collective_id=0, has_side_effects=True, vmem_limit_bytes=VMEM_BYTES
        ),
    )(tokens, expert_ids.T, gate_vals.T, w_gate, w_up, w_down)


def routing(expert_ids, gate_vals, held_count, capacity):
    first = lax.axis_index("blk") * held_count
    top_k = expert_ids.shape[1]
    both = jnp.concatenate((expert_ids.astype(jnp.float32), gate_vals), axis=1)
    both = lax.all_gather(both, "blk", axis=0, tiled=False)
    ids, gates = both[:, :, :top_k].astype(jnp.int32), both[:, :, top_k:]
    mine = first + jnp.arange(held_count, dtype=jnp.int32)
    match = ids[:, None, :, :] == mine[None, :, None, None]
    member = jnp.any(match, axis=3)
    weight = jnp.sum(jnp.where(match, gates[:, None], 0.0), axis=3)
    tok_rows = ids.shape[1]
    earlier = jnp.triu(jnp.ones((tok_rows, tok_rows), jnp.float32), 1)
    position = jnp.einsum(
        "bht,tu->bhu", member.astype(jnp.bfloat16), earlier.astype(jnp.bfloat16),
        preferred_element_type=jnp.float32,
    )
    slots = jnp.arange(capacity, dtype=jnp.int32).astype(jnp.float32)
    hot = member[:, :, None, :] & (position[:, :, None, :] == slots[None, None, :, None])
    return hot.astype(jnp.bfloat16), jnp.where(hot, weight[:, :, None, :], 0.0)


def local(tokens, expert_ids, gate_vals, w_gate, w_up, w_down):
    blk_size = lax.axis_size("blk")
    tok_rows, width_dev = tokens.shape
    top_k = expert_ids.shape[1]
    held_count = w_gate.shape[0]
    capacity = 2 * tok_rows * top_k // (held_count * blk_size)
    hot, weighted = routing(expert_ids, gate_vals, held_count, capacity)
    everyone = lax.all_gather(tokens, "blk", axis=0, tiled=False)
    routed = jnp.einsum("bhpt,btd->hbpd", hot, everyone, preferred_element_type=jnp.float32)
    routed = routed.astype(jnp.bfloat16).reshape(held_count, blk_size * capacity, width_dev)
    gate_part = jnp.einsum("emd,edf->emf", routed, w_gate, preferred_element_type=jnp.float32)
    up_part = jnp.einsum("emd,edf->emf", routed, w_up, preferred_element_type=jnp.float32)
    both = jnp.stack((gate_part, up_part), axis=0)
    summed = lax.psum_scatter(both, "dp", scatter_dimension=2, tiled=True)
    hidden = (jax.nn.silu(summed[0]) * summed[1]).astype(jnp.bfloat16)
    hidden = lax.all_gather(hidden, "dp", axis=1, tiled=True)
    result = jnp.einsum("emf,edf->emd", hidden, w_down, preferred_element_type=jnp.float32)
    result = result.astype(jnp.bfloat16).reshape(held_count, blk_size, capacity, width_dev)
    high = weighted.astype(jnp.bfloat16)
    low = (weighted - high.astype(jnp.float32)).astype(jnp.bfloat16)
    partial = jnp.einsum(
        "bhpt,hbpd->btd", high, result, preferred_element_type=jnp.float32
    ) + jnp.einsum("bhpt,hbpd->btd", low, result, preferred_element_type=jnp.float32)
    partial = partial.astype(jnp.bfloat16).reshape(blk_size * tok_rows, width_dev)
    return lax.psum_scatter(partial, "blk", scatter_dimension=0, tiled=True)


def choose(tokens, expert_ids, gate_vals, w_gate, w_up, w_down):
    n_blk, held = lax.axis_size("blk"), w_gate.shape[0]
    capacity = 2 * tokens.shape[0] * expert_ids.shape[1] // (held * n_blk)
    fits = lax.axis_size("dp") == 4 and held == 2 and n_blk == 8 and capacity % 32 == 0
    fits = fits and w_gate.shape[2] % (2 * TILE) == 0 and tokens.shape[1] % DOWN == 0
    body = fused if fits else local
    return body(tokens, expert_ids, gate_vals, w_gate, w_up, w_down)


def solution(mesh):
    return jax.shard_map(
        choose,
        mesh=mesh,
        in_specs=(
            P("blk", "dp"),
            P("blk", None),
            P("blk", None),
            P("blk", "dp", None),
            P("blk", "dp", None),
            P("blk", "dp", None),
        ),
        out_specs=P("blk", "dp"),
        check_vma=False,
    )
```

```python
import functools

import jax
import jax.numpy as jnp
from jax import lax
from jax.experimental import pallas as pl
from jax.experimental.pallas import tpu as pltpu
from jax.sharding import PartitionSpec as P

MESH = pl.DeviceIdType.MESH
VMEM_BYTES = 66_000_000
TILE = 384
DOWN = 256
RING = 4
SPLIT = 512
ORDER = (0, 2, 4, 5, 7, 6, 1, 3)


def flip(a, m, size):
    total, unit = 0, 1
    while unit < size:
        total = total + lax.rem(lax.div(a, unit) + lax.div(m, unit), 2) * unit
        unit *= 2
    return total


def fused_kernel(
    n_blk, tok_hbm, ids_hbm, gates_hbm, wg_hbm, wu_hbm, wd_hbm, out_ref,
    wg, wu, wd, everyone, routed, part, near, far_out, far_in, hidden, rows_out,
    outgoing, arrived, hold, acc, ids_ref, gates_ref, info, high, low, hot,
    w_sem, tok_s, tok_r, near_s, near_r, far_s, far_r, hy_s, hy_r, hc_s, hc_r, hf_s, hf_r, ret_s, ret_r, info_s, info_r,
):
    blk = lax.axis_index("blk")
    dp = lax.axis_index("dp")
    y, c = lax.div(dp, 2), lax.rem(dp, 2)
    mate = (blk, y * 2 + (1 - c))
    across = (blk, (1 - y) * 2 + c)
    held, width, ff = wg.shape
    cols = ff // 2
    half = near.shape[2]
    cap = 2 * half
    units = held * n_blk

    def copy(src, dst, send, recv, device):
        return pltpu.make_async_remote_copy(
            src_ref=src, dst_ref=dst, send_sem=send, recv_sem=recv,
            device_id=device, device_id_type=MESH,
        )

    def peer(m):
        return (flip(blk, m, n_blk), dp)

    def mask_of(i):
        m = 0
        for k in range(1, n_blk):
            m = jnp.where(i == k, ORDER[k], m)
        return m

    def hop(m, k, to, have):
        tok, ids = (everyone.at[have or 0], info.at[have or 0])
        return (
            copy(tok, everyone.at[m], tok_s.at[k], tok_r.at[m], peer(to)),
            copy(ids, info.at[m], info_s.at[k], info_r.at[m], peer(to)),
        )

    def send(hops):
        for part_of in hops:
            part_of.start()

    def sent(hops):
        for part_of in hops:
            part_of.wait_send()

    def received(m):
        for part_of in hop(m, m, m, None):
            part_of.wait_recv()

    def direct(m):
        return hop(m, m, m, None)

    def relay_hop(have, m, k, to):
        return hop(m, k, to, have)

    def onward(m):
        return hop(m + 1, m + 1, 1, m)

    def middle():
        return hop(6, 0, 6, None)

    relays = ((2, 4, 4, 6), (6, 4, 6, 2), (4, 6, n_blk, 2))

    def near_copy(u, which):
        k, span = lax.rem(u, 2), slice(which * cols, (which + 1) * cols)
        return copy(
            part.at[0, :, :, span], near.at[u, :, :, span], near_s.at[k, which], near_r.at[k, which], mate
        )

    def far_copy(u, which):
        k, span = lax.rem(u, RING), slice(which * cols, (which + 1) * cols)
        return copy(
            far_out.at[u, :, span], far_in.at[u, :, span], far_s.at[k, which], far_r.at[k, which], across
        )

    def hidden_far(u):
        return copy(hidden.at[u, c, y], hidden.at[u, c, y], hy_s.at[lax.rem(u, RING)], hy_r.at[lax.rem(u, RING)], across)

    def hidden_near(u):
        return copy(hidden.at[u, c, y], hidden.at[u, c, y], hc_s.at[lax.rem(u, RING)], hc_r.at[lax.rem(u, RING)], mate)

    def hidden_onward(u):
        return copy(hidden.at[u, c, 1 - y], hidden.at[u, c, 1 - y], hf_s.at[lax.rem(u, RING)], hf_r.at[lax.rem(u, RING)], mate)

    def ret_copy(m):
        to = jnp.where((lax.rem(m, 2) == 1) & (m > 3), 1, m)
        return copy(outgoing.at[m], arrived.at[m], ret_s.at[m], ret_r.at[m], peer(to))

    spans = ((0, SPLIT), (SPLIT, width))

    def ret_part(m, k):
        d0, d1 = spans[k]
        sem = m if k == 0 else jnp.where(m == 1, 0, n_blk)
        return copy(
            outgoing.at[m, :, d0:d1], arrived.at[m, :, d0:d1], ret_s.at[sem], ret_r.at[sem], peer(m)
        )

    def load(k, h):
        hbm, vmem = ((wg_hbm, wg), (wu_hbm, wu), (wd_hbm, wd))[k]
        return pltpu.make_async_copy(hbm.at[h], vmem.at[h], w_sem.at[k, h])

    def columns(side):
        return pl.multiple_of(jnp.where(c == side, cols, 0), 128)

    def load_side(k, side):
        hbm, vmem = ((wg_hbm, wg), (wu_hbm, wu))[k]
        span = (0, slice(None), pl.ds(columns(side), cols))
        return pltpu.make_async_copy(hbm.at[span], vmem.at[span], w_sem.at[3 + k, side])

    inputs = [
        pltpu.make_async_copy(ids_hbm, ids_ref, w_sem.at[5, 0]),
        pltpu.make_async_copy(gates_hbm, gates_ref, w_sem.at[5, 1]),
        pltpu.make_async_copy(tok_hbm, everyone.at[0], w_sem.at[2, 0]),
    ]
    for load_in in inputs:
        load_in.start()
    for side in range(2):
        for k in range(2):
            load_side(k, side).start()

    inner = lax.rem(lax.div(lax.div(blk, 2) + 1, 2), 2) == 1
    barrier = pltpu.get_barrier_semaphore()
    for device in (peer(2), peer(1), mate, across):
        pl.semaphore_signal(barrier, inc=1, device_id=device, device_id_type=MESH)

    @pl.when(inner)
    def _():
        pl.semaphore_signal(barrier, inc=1, device_id=peer(6), device_id_type=MESH)

    tok_rows = everyone.shape[1]
    top_k = ids_ref.shape[0]
    lines = info.shape[1] // 2
    for load_in in inputs:
        load_in.wait()
    info[0] = jnp.full(info.shape[1:], -1.0, jnp.float32)
    info[0, :top_k] = ids_ref[...].astype(jnp.float32)
    info[0, lines:lines + top_k] = gates_ref[...]
    pl.semaphore_wait(barrier, 4 + jnp.where(inner, 1, 0))

    send(direct(2))
    send(direct(1))

    @pl.when(inner)
    def _():
        send(middle())


    def slots_of(m):
        square = (tok_rows, tok_rows)
        before = lax.broadcasted_iota(jnp.int32, square, 0) < lax.broadcasted_iota(jnp.int32, square, 1)
        before = jnp.where(before, 1.0, 0.0).astype(jnp.bfloat16)
        slot = lax.broadcasted_iota(jnp.int32, (cap, tok_rows), 0).astype(jnp.float32)
        ids, gates = info[m, :lines], info[m, lines:]
        for h in range(held):
            match = ids == (held * blk + h).astype(jnp.float32)
            member = jnp.sum(jnp.where(match, 1.0, 0.0), axis=0, keepdims=True)
            weight = jnp.sum(jnp.where(match, gates, 0.0), axis=0, keepdims=True)
            wide = jnp.broadcast_to(member, (16, tok_rows)).astype(jnp.bfloat16)
            position = jnp.dot(wide, before, preferred_element_type=jnp.float32)[0:1]
            taken = (slot == position) & (member > 0.5)
            weighted = jnp.where(taken, weight, 0.0)
            top = weighted.astype(jnp.bfloat16)
            span = slice(h * cap, (h + 1) * cap)
            high[m, span, :] = top
            low[m, span, :] = (weighted - top.astype(jnp.float32)).astype(jnp.bfloat16)
            hot[h] = jnp.where(taken, 1.0, 0.0).astype(jnp.bfloat16)

    def project(u):
        i, h = lax.div(u, held), lax.rem(u, held)
        m = mask_of(i)

        @pl.when(h == 0)
        def _():
            @pl.when(i > 0)
            def _():
                @pl.when(m != 6)
                def _():
                    received(m)

                @pl.when(m == 2)
                def _():
                    @pl.when(inner)
                    def _():
                        send(relay_hop(*relays[0]))
                        received(6)
                        send(relay_hop(*relays[1]))

                    send(onward(2))

                @pl.when(m == 4)
                def _():
                    @pl.when(inner)
                    def _():
                        send(relay_hop(*relays[2]))

                    send(onward(4))

                @pl.when(m == 5)
                def _():
                    @pl.when(jnp.logical_not(inner))
                    def _():
                        received(6)

                    send(onward(6))

            slots_of(m)

        routed[...] = jnp.dot(
            hot[h], everyone[m], preferred_element_type=jnp.float32
        ).astype(jnp.bfloat16)

        @pl.when(u == 1)
        def _():
            load(0, 1).wait()
            load(1, 1).wait()
            load(2, 0).start()
            load(2, 1).start()

        for side in range(2):
            first = jnp.where(c == side, cols, 0)
            for which, w in enumerate((wg, wu)):
                @pl.when(u == 0)
                def _():
                    load_side(which, side).wait()
                    if side == 0 and which == 1:
                        load(0, 1).start()
                        load(1, 1).start()

                for f in range(0, cols, TILE):
                    at = pl.multiple_of(first + f, 128)
                    got = jnp.dot(
                        routed[...], w[h, :, pl.ds(at, TILE)], preferred_element_type=jnp.float32
                    )
                    span = slice(which * cols + f, which * cols + f + TILE)
                    part[side, 0, :, span] = got[:half]
                    part[side, 1, :, span] = got[half:]
                if side == 0:
                    near_copy(u, which).start()

    def join(u):
        for which in range(2):
            span = slice(which * cols, (which + 1) * cols)
            near_copy(u, which).wait()
            far_out[u, :, span] = (part[1, 1 - y, :, span] + near[u, 1 - y, :, span]).astype(jnp.bfloat16)
            far_copy(u, which).start()
        near[u, y] = near[u, y] + part[1, y]

    def activate(u):
        far_copy(u, 0).wait()
        far_copy(u, 1).wait()
        gate = near[u, y, :, :cols] + far_in[u, :, :cols].astype(jnp.float32)
        up = near[u, y, :, cols:] + far_in[u, :, cols:].astype(jnp.float32)
        hidden[u, c, y] = (gate / (1.0 + jnp.exp(-gate)) * up).astype(jnp.bfloat16)
        hidden_far(u).start()
        hidden_near(u).start()

    def relay(u):
        hidden_far(u).wait()
        hidden_onward(u).start()

    def finish(u):
        i, h = lax.div(u, held), lax.rem(u, held)
        m = mask_of(i)

        @pl.when(i == 0)
        def _():
            load(2, h).wait()

        hidden_near(u).wait()
        hidden_onward(u).wait()
        rows = jnp.concatenate([hidden[u, k].reshape(cap, cols) for k in range(2)], axis=1)
        def down(d0, d1):
            for d in range(d0, d1, DOWN):
                rows_out[h, :, d:d + DOWN] = lax.dot_general(
                    rows, wd[h, d:d + DOWN, :], (((1,), (1,)), ((), ())),
                    preferred_element_type=jnp.float32,
                ).astype(jnp.bfloat16)

        def mix(d0, d1):
            both = rows_out[:, :, d0:d1].reshape(held * cap, d1 - d0)
            over_slots = (((0,), (0,)), ((), ()))
            weights = jnp.concatenate([high[m], low[m]], axis=0)
            twice = jnp.concatenate([both, both], axis=0)
            return lax.dot_general(weights, twice, over_slots, preferred_element_type=jnp.float32)

        last = (m == 1) | (m == 3)

        @pl.when((h < held - 1) | jnp.logical_not(last))
        def _():
            down(0, width)

        @pl.when((h == held - 1) & last)
        def _():
            for k, (d0, d1) in enumerate(spans):
                down(d0, d1)
                outgoing[m, :, d0:d1] = mix(d0, d1).astype(jnp.bfloat16)
                ret_part(m, k).start()

        @pl.when((h == held - 1) & jnp.logical_not(last))
        def _():
            mixed = mix(0, width)

            @pl.when(m == 0)
            def _():
                acc[...] = mixed

            @pl.when((m > 2) & (lax.rem(m, 2) == 0))
            def _():
                hold[lax.div(m, 2) - 2] = mixed

            @pl.when((lax.rem(m, 2) == 1) | (m == 2))
            def _():
                outgoing[m] = mixed.astype(jnp.bfloat16)
                ret_copy(m).start()

    def merge(u):
        m = jnp.where(u == 9, 4, 6)

        @pl.when((u == 9) | (u == 11))
        def _():
            ret_copy(m + 1).wait_recv()
            total = hold[lax.div(m, 2) - 2] + arrived[m + 1].astype(jnp.float32)
            outgoing[m] = total.astype(jnp.bfloat16)
            ret_copy(m).start()

    def early(u):
        @pl.when(u == units - 3)
        def _():
            finish(u)

    def late(u):
        @pl.when(u != units - 3)
        def _():
            finish(u)

    stages = (
        (1, join), (4, early), (2, activate), (0, project), (3, relay), (4, late), (4, merge),
    )

    def step(s, carry):
        for lag, stage in stages:
            @pl.when((s >= lag) & (s - lag < units))
            def _():
                stage(s - lag)
        return carry

    lax.fori_loop(0, units + 4, step, 0)

    for m in (1, 2):
        sent(direct(m))
    for m in (2, 4, 6):
        sent(onward(m))

    @pl.when(inner)
    def _():
        sent(middle())
        for args in relays:
            sent(relay_hop(*args))

    for m in (2, 4, 6):
        ret_copy(m).wait_recv()
    acc[...] = acc[...] + sum(arrived[m].astype(jnp.float32) for m in (2, 4, 6))
    for m in (2, 4, 5, 6, 7):
        ret_copy(m).wait_send()
    for k in range(2):
        ret_part(1, k).wait_send()
    for k in range(2):
        ret_part(1, k).wait_recv()
    acc[...] = acc[...] + arrived[1].astype(jnp.float32)
    for k, (d0, d1) in enumerate(spans):
        ret_part(3, k).wait_recv()
        out_ref[:, d0:d1] = (acc[:, d0:d1] + arrived[3, :, d0:d1].astype(jnp.float32)).astype(jnp.bfloat16)
    for k in range(2):
        ret_part(3, k).wait_send()


def fused(tokens, expert_ids, gate_vals, w_gate, w_up, w_down):
    n_blk = lax.axis_size("blk")
    tok_rows, width = tokens.shape
    held, _, ff = w_gate.shape
    capacity = 2 * tok_rows * expert_ids.shape[1] // (held * n_blk)
    half, units = capacity // 2, held * n_blk
    top_k = expert_ids.shape[1]
    lines = top_k + -top_k % 8
    bf, f32 = jnp.bfloat16, jnp.float32
    dma = pltpu.SemaphoreType.DMA
    counts = [n_blk + 1, n_blk, (2, 2), (2, 2)] + [(RING, 2)] * 2 + [RING] * 6 + [n_blk + 1] * 3 + [n_blk]
    vmem = pl.BlockSpec(memory_space=pltpu.VMEM)
    anywhere = pl.BlockSpec(memory_space=pl.ANY)
    return pl.pallas_call(
        functools.partial(fused_kernel, n_blk),
        out_shape=pltpu.VMEM((tok_rows, width), bf),
        in_specs=[anywhere] * 6,
        out_specs=vmem,
        scratch_shapes=[
            pltpu.VMEM(w_gate.shape, bf),
            pltpu.VMEM(w_up.shape, bf),
            pltpu.VMEM(w_down.shape, bf),
            pltpu.VMEM((n_blk, tok_rows, width), bf),
            pltpu.VMEM((capacity, width), bf),
            pltpu.VMEM((2, 2, half, ff), f32),
            pltpu.VMEM((units, 2, half, ff), f32),
            pltpu.VMEM((units, half, ff), bf),
            pltpu.VMEM((units, half, ff), bf),
            pltpu.VMEM((units, 2, 2, half, ff // 2), bf),
            pltpu.VMEM((held, capacity, width), bf),
            pltpu.VMEM((n_blk, tok_rows, width), bf),
            pltpu.VMEM((n_blk, tok_rows, width), bf),
            pltpu.VMEM((n_blk // 2 - 2, tok_rows, width), f32),
            pltpu.VMEM((tok_rows, width), f32),
            pltpu.VMEM((top_k, tok_rows), jnp.int32),
            pltpu.VMEM((top_k, tok_rows), f32),
            pltpu.VMEM((n_blk, 2 * lines, tok_rows), f32),
            pltpu.VMEM((n_blk, held * capacity, tok_rows), bf),
            pltpu.VMEM((n_blk, held * capacity, tok_rows), bf),
            pltpu.VMEM((held, capacity, tok_rows), bf),
            dma((6, 2)),
        ] + [dma(count if isinstance(count, tuple) else (count,)) for count in counts],
        compiler_params=pltpu.CompilerParams(
            collective_id=0, has_side_effects=True, vmem_limit_bytes=VMEM_BYTES
        ),
    )(tokens, expert_ids.T, gate_vals.T, w_gate, w_up, w_down)


def routing(expert_ids, gate_vals, held_count, capacity):
    first = lax.axis_index("blk") * held_count
    top_k = expert_ids.shape[1]
    both = jnp.concatenate((expert_ids.astype(jnp.float32), gate_vals), axis=1)
    both = lax.all_gather(both, "blk", axis=0, tiled=False)
    ids, gates = both[:, :, :top_k].astype(jnp.int32), both[:, :, top_k:]
    mine = first + jnp.arange(held_count, dtype=jnp.int32)
    match = ids[:, None, :, :] == mine[None, :, None, None]
    member = jnp.any(match, axis=3)
    weight = jnp.sum(jnp.where(match, gates[:, None], 0.0), axis=3)
    tok_rows = ids.shape[1]
    earlier = jnp.triu(jnp.ones((tok_rows, tok_rows), jnp.float32), 1)
    position = jnp.einsum(
        "bht,tu->bhu", member.astype(jnp.bfloat16), earlier.astype(jnp.bfloat16),
        preferred_element_type=jnp.float32,
    )
    slots = jnp.arange(capacity, dtype=jnp.int32).astype(jnp.float32)
    hot = member[:, :, None, :] & (position[:, :, None, :] == slots[None, None, :, None])
    return hot.astype(jnp.bfloat16), jnp.where(hot, weight[:, :, None, :], 0.0)


def local(tokens, expert_ids, gate_vals, w_gate, w_up, w_down):
    blk_size = lax.axis_size("blk")
    tok_rows, width_dev = tokens.shape
    top_k = expert_ids.shape[1]
    held_count = w_gate.shape[0]
    capacity = 2 * tok_rows * top_k // (held_count * blk_size)
    hot, weighted = routing(expert_ids, gate_vals, held_count, capacity)
    everyone = lax.all_gather(tokens, "blk", axis=0, tiled=False)
    routed = jnp.einsum("bhpt,btd->hbpd", hot, everyone, preferred_element_type=jnp.float32)
    routed = routed.astype(jnp.bfloat16).reshape(held_count, blk_size * capacity, width_dev)
    gate_part = jnp.einsum("emd,edf->emf", routed, w_gate, preferred_element_type=jnp.float32)
    up_part = jnp.einsum("emd,edf->emf", routed, w_up, preferred_element_type=jnp.float32)
    both = jnp.stack((gate_part, up_part), axis=0)
    summed = lax.psum_scatter(both, "dp", scatter_dimension=2, tiled=True)
    hidden = (jax.nn.silu(summed[0]) * summed[1]).astype(jnp.bfloat16)
    hidden = lax.all_gather(hidden, "dp", axis=1, tiled=True)
    result = jnp.einsum("emf,edf->emd", hidden, w_down, preferred_element_type=jnp.float32)
    result = result.astype(jnp.bfloat16).reshape(held_count, blk_size, capacity, width_dev)
    high = weighted.astype(jnp.bfloat16)
    low = (weighted - high.astype(jnp.float32)).astype(jnp.bfloat16)
    partial = jnp.einsum(
        "bhpt,hbpd->btd", high, result, preferred_element_type=jnp.float32
    ) + jnp.einsum("bhpt,hbpd->btd", low, result, preferred_element_type=jnp.float32)
    partial = partial.astype(jnp.bfloat16).reshape(blk_size * tok_rows, width_dev)
    return lax.psum_scatter(partial, "blk", scatter_dimension=0, tiled=True)


def choose(tokens, expert_ids, gate_vals, w_gate, w_up, w_down):
    n_blk, held = lax.axis_size("blk"), w_gate.shape[0]
    capacity = 2 * tokens.shape[0] * expert_ids.shape[1] // (held * n_blk)
    fits = lax.axis_size("dp") == 4 and held == 2 and n_blk == 8 and capacity % 32 == 0
    fits = fits and w_gate.shape[2] % (2 * TILE) == 0 and tokens.shape[1] % DOWN == 0
    body = fused if fits else local
    return body(tokens, expert_ids, gate_vals, w_gate, w_up, w_down)


def solution(mesh):
    return jax.shard_map(
        choose,
        mesh=mesh,
        in_specs=(
            P("blk", "dp"),
            P("blk", None),
            P("blk", None),
            P("blk", "dp", None),
            P("blk", "dp", None),
            P("blk", "dp", None),
        ),
        out_specs=P("blk", "dp"),
        check_vma=False,
    )
```
